512 devices in a mesh: rows: 128 (over z, x, core), cols: 4 (over y).
Axes of the slice: x: 4, y: 4, z: 16, core: 2. Of those that a mesh axis runs over, the one named last changes fastest.
Arguments:
- basis_rows: bfloat16 [327680, 512], P('rows', 'cols'), may hold values from -24 to 24
- stiff_blocks: bfloat16 [2560, 3, 128, 128], P('rows'), may hold values from -0.3125 to 0.3125
- block_neighbors: int32 [2560, 3], P('rows'), may hold values from 0 to 2559, as said below
- vertex_mass: float32 [327680], P('rows'), may hold values from 0.4 to 7.5
- rotation: bfloat16 [512, 512], replicated, may hold values from -0.25 to 0.25
Outputs:
- new_basis: bfloat16 [327680, 512], P('rows', 'cols')
- stiff_image: bfloat16 [327680, 512], P('rows', 'cols')
- stiff_gram: float32 [512, 512], P('rows', 'cols')
- mass_gram: float32 [512, 512], P('rows', 'cols')
The draws below stay inside these ranges and needn't reach their ends.
Inputs may be any that keep to these rules, and one draw needn't show every extreme that they name: `block_neighbors`: entry 0 of block row b is b itself; every entry of block row b lies within 8 of b.
All inputs are finite; a program needn't handle non-finite values.
Results may differ from the reference program's by a relative error of at most 0.008.
Values may be sent and summed in bfloat16 or wider, within the bound.
A program may use at most 64 MiB of HBM per device.

```python
import math
import jax
import jax.numpy as jnp
from jax import lax

K = 512
B = 128
NB = 3
BAND = 8
NBLK = 2560
NV = 327680


def draw_block_neighbors(key, part):
    row_index = jnp.arange(NBLK, dtype=jnp.int32)[:, None]
    offsets = jax.random.randint(key, (NBLK, NB), -BAND, BAND + 1, dtype=jnp.int32)
    column = jnp.arange(NB, dtype=jnp.int32)[None, :]
    offsets = jnp.where(column == 0, 0, offsets)
    return jnp.clip(row_index + offsets, 0, NBLK - 1).astype(jnp.int32)


def draw_vertex_mass(key, part):
    position = jnp.arange(NV, dtype=jnp.float32) / (NV - 1)
    ramp = 1.0 + 2.0 * position
    rough = jnp.exp(jax.random.uniform(key, (NV,), jnp.float32, math.log(0.5), math.log(2.0)))
    return (rough * ramp).astype(jnp.float32)


def raised(drawn, stream_key, source, target, parts, factor):
    def block_of(dim):
        return (jnp.arange(drawn.shape[dim]) // (drawn.shape[dim] // parts)).reshape((-1,) + (1,) * (drawn.ndim - 1 - dim))

    one_side = jax.random.permutation(stream_key, parts)[block_of(target)]
    far = (block_of(target) + parts // 2) % parts
    return jnp.where((block_of(source) == one_side) | (block_of(source) == far), factor * drawn, drawn)


def shard_levels(stream_key, shape, split, low, largest):
    def one(dim, shards_of):
        steps = jax.random.uniform(jax.random.fold_in(jax.random.fold_in(stream_key, 6), dim), (shards_of,), jnp.float32, low / len(split), largest / len(split))
        return jnp.repeat(jnp.exp(steps), shape[dim] // shards_of).reshape((-1,) + (1,) * (len(shape) - dim - 1))

    factor_of = one(*split[0])
    for cut in split[1:]:
        factor_of = factor_of * one(*cut)
    return factor_of


def scatter_about(rng, dims, width, reach, shards=(), kind=jnp.bfloat16):
    loudness = shard_levels(rng, dims, shards, -0.22, 0.18) if shards else 1.0
    array = jax.random.normal(rng, dims, jnp.float32) * width * loudness
    return jnp.minimum(jnp.maximum(array, -reach), reach).astype(kind)


def bell_draw_with(stream_key, extent, width, bound, shards, heavy, kind=jnp.bfloat16):
    array = width * jax.random.normal(stream_key, extent, jnp.float32)
    if shards:
        array = array * shard_levels(stream_key, extent, shards, -0.22, 0.18)
    return jnp.clip(raised(array, jax.random.fold_in(stream_key, 3), *heavy), -bound, bound).astype(kind)


def setup_inputs(seed: int = 0) -> dict:
    keys = jax.random.split(jax.random.key(seed), 6)
    basis_rows = bell_draw_with(keys[0], (NV, K), 1.0, 24.0, ((0, 128), (1, 4)), (0, 1, 128, 5.5))
    stiff_blocks = scatter_about(keys[1], (NBLK, NB, B, B), (B * NB) ** -0.5, 0.3125, ((0, 128),))
    block_neighbors = draw_block_neighbors(jax.random.fold_in(keys[5], 71), 0)
    vertex_mass = draw_vertex_mass(jax.random.fold_in(keys[5], 71), 0)
    rotation = scatter_about(keys[4], (K, K), K ** -0.5, 0.25)
    return dict(basis_rows=basis_rows, stiff_blocks=stiff_blocks, block_neighbors=block_neighbors, vertex_mass=vertex_mass, rotation=rotation)


def reference(basis_rows, stiff_blocks, block_neighbors, vertex_mass, rotation):
    blocks = basis_rows.reshape(NBLK, B, K).astype(jnp.float32)
    image_blocks = jnp.zeros((NBLK, B, K), jnp.float32)
    for slot in range(NB):
        source = blocks[block_neighbors[:, slot].astype(jnp.int32)]
        image_blocks = image_blocks + jnp.einsum('kij,kjc->kic', stiff_blocks[:, slot].astype(jnp.float32), source, precision=lax.Precision.HIGHEST)
    stiff_rows = image_blocks.reshape(NV, K)
    half_image = stiff_rows.astype(jnp.bfloat16)
    weighted = (vertex_mass[:, None] * basis_rows.astype(jnp.float32)).astype(jnp.bfloat16)
    stiff_gram = jnp.dot(basis_rows.T, half_image, preferred_element_type=jnp.float32) / NV
    mass_gram = jnp.dot(basis_rows.T, weighted, preferred_element_type=jnp.float32) / NV
    turned = jnp.dot(basis_rows, rotation, preferred_element_type=jnp.float32)
    squares = lax.optimization_barrier(jnp.sum(vertex_mass[:, None] * turned * turned, axis=0)) / NV
    scale = 1.0 / jnp.sqrt(squares)
    new_basis = (turned * scale).astype(jnp.bfloat16)
    rotated_image = jnp.dot(stiff_rows, rotation.astype(jnp.float32), precision=lax.Precision.HIGHEST)
    stiff_image = (rotated_image * scale).astype(jnp.bfloat16)
    return (new_basis, stiff_image, stiff_gram, mass_gram)
```

```python
import jax
import jax.numpy as jnp
from jax import lax
from jax.sharding import Mesh
from jax.sharding import PartitionSpec as P

BAND = 8
ROWS = ("rows_0", "rows_1", "rows_2")


def with_halo(block, sides, width):
    for axis, dim in sides:
        count = lax.axis_size(axis)
        forward = [(i, i + 1) for i in range(count - 1)]
        backward = [(target, source) for source, target in forward]
        low = lax.ppermute(
            lax.slice_in_dim(block, block.shape[dim] - width, None, axis=dim), axis, forward
        )
        high = lax.ppermute(lax.slice_in_dim(block, 0, width, axis=dim), axis, backward)
        block = jnp.concatenate([low, block, high], axis=dim)
    return block


def from_everyone(value, axis):
    size = lax.axis_size(axis)
    return lax.all_to_all(
        jnp.broadcast_to(value[None], (size, *value.shape)), axis, 0, 0, tiled=True
    )


def laid_out(tiles, dim):
    shape = list(tiles.shape[1:])
    shape[dim] *= tiles.shape[0]
    return jnp.moveaxis(tiles, 0, dim).reshape(shape)


def gather_directly(value, axis, dim):
    tiles = from_everyone(value, axis)
    return laid_out(tiles, dim)


def cut_along(value, dim, size):
    shape = value.shape
    tiles = value.reshape(*shape[:dim], size, shape[dim] // size, *shape[dim + 1 :])
    return jnp.moveaxis(tiles, dim, 0)


def sent_and_summed(value, axis, dim):
    size = lax.axis_size(axis)
    tiles = lax.all_to_all(cut_along(value, dim, size), axis, 0, 0, tiled=True)
    return jnp.sum(tiles, axis=0)


def apply_blocks(padded, stiff_blocks, block_neighbors, first_block):
    block_count = stiff_blocks.shape[0]
    block_size = stiff_blocks.shape[2]
    col_width = padded.shape[1]
    tiles = padded.reshape(block_count + 2 * BAND, block_size, col_width)
    local_index = block_neighbors - first_block + BAND
    source = tiles[local_index]
    result = jnp.einsum(
        "knij,knjc->kic", stiff_blocks, source, preferred_element_type=jnp.float32
    )
    return result.reshape(block_count * block_size, col_width)


def body(basis_rows, stiff_blocks, block_neighbors, vertex_mass, rotation):
    row_count = lax.axis_size(ROWS)
    row_place = lax.axis_index(ROWS)
    col_place = lax.axis_index("cols")
    local_rows, col_width = basis_rows.shape
    block_count = stiff_blocks.shape[0]
    block_size = stiff_blocks.shape[2]
    vertices = local_rows * row_count
    first_block = row_place * block_count
    near, far = "rows_2", ("rows_0", "rows_1")
    local_turn = lax.dynamic_slice_in_dim(rotation, col_place * col_width, col_width, 1)
    padded = with_halo(basis_rows, ((ROWS, 0),), BAND * block_size)
    piece = gather_directly(basis_rows, "cols", 1)
    stiff_rows = apply_blocks(padded, stiff_blocks, block_neighbors, first_block)
    half_image = stiff_rows.astype(jnp.bfloat16)
    weighted = (vertex_mass[:, None] * basis_rows.astype(jnp.float32)).astype(jnp.bfloat16)
    turned = jnp.dot(piece, local_turn, preferred_element_type=jnp.float32)
    turned_half = turned.astype(jnp.bfloat16)
    rimmed = with_halo(turned_half, ((ROWS, 0),), BAND * block_size)
    stiff_part = lax.dot_general(
        piece, half_image, (((0,), (0,)), ((), ())), preferred_element_type=jnp.float32
    )
    mass_part = lax.dot_general(
        piece, weighted, (((0,), (0,)), ((), ())), preferred_element_type=jnp.float32
    )
    squares = jnp.sum(vertex_mass[:, None] * turned * turned, axis=0)
    parts = jnp.concatenate([stiff_part, mass_part], axis=1)
    wide = jnp.zeros((2 * col_width,), jnp.float32).at[:col_width].set(squares)
    tiles = cut_along(parts, 0, lax.axis_size(far))
    nearer = sent_and_summed(
        jnp.concatenate(
            [
                tiles.reshape(lax.axis_size(far), 2, -1, 2 * col_width),
                jnp.broadcast_to(wide, (lax.axis_size(far), 2, 1, 2 * col_width)),
            ],
            axis=2,
        ).reshape(lax.axis_size(far), -1, 2 * col_width),
        near,
        1,
    )
    arrived = lax.all_to_all(nearer, far, split_axis=0, concat_axis=0, tiled=True)
    grams = arrived.sum(axis=0) / vertices
    product = apply_blocks(rimmed, stiff_blocks, block_neighbors, first_block)
    scale = lax.rsqrt(grams[-1, :col_width])
    new_basis = (turned * scale).astype(jnp.bfloat16)
    stiff_image = (product * scale).astype(jnp.bfloat16)
    return (new_basis, stiff_image, grams[:-1, :col_width], grams[:-1, col_width:])


def solution(mesh):
    split = Mesh(
        mesh.devices.reshape(16, 4, 2, mesh.shape["cols"]), ("rows_0", "rows_1", "rows_2", "cols")
    )
    in_specs = (P(ROWS, "cols"), P(ROWS, None, None, None), P(ROWS, None), P(ROWS), P())
    out_specs = (P(ROWS, "cols"), P(ROWS, "cols"), P(ROWS, "cols"), P(ROWS, "cols"))
    return jax.shard_map(body, mesh=split, in_specs=in_specs, out_specs=out_specs, check_vma=False)
```

```python
import functools

import jax
import jax.numpy as jnp
from jax import lax
from jax.experimental import pallas as pl
from jax.experimental.pallas import tpu as pltpu
from jax.sharding import Mesh
from jax.sharding import PartitionSpec as P

BAND = 8
ROWS = ("rows_0", "rows_1", "rows_2")
MESH = pl.DeviceIdType.MESH
F32 = jnp.float32
BF16 = jnp.bfloat16
OWN, LEFT, RIGHT, FAR = 0, 1, 2, 3


def transposed_dot(left, right):
    return lax.dot_general(left, right, (((0,), (0,)), ((), ())), preferred_element_type=F32)


def kernel(
    sizes,
    nb_ref,
    basis_ref,
    blocks_ref,
    mass_ref,
    rot_ref,
    basis_out,
    image_out,
    stiff_out,
    mass_out,
    padded,
    others,
    rimmed,
    turned,
    product,
    mass_col,
    weights,
    blocks,
    turn,
    gram,
    gram_core,
    gram_x,
    gram_x_in,
    gram_z,
    gram_z_in,
    tile_mine,
    tile_in,
    sq_own,
    sq_core,
    sq_x,
    sq_x_in,
    sq_z,
    sq_z_in,
    load_sem,
    y_send,
    y_recv,
    halo_send,
    halo_recv,
    core_send,
    core_recv,
    x_send,
    x_recv,
    z_send,
    z_recv,
):
    nz, nx, ny, count, size, width, parts = sizes
    z, x, k = (lax.axis_index(a) for a in ROWS)
    y = lax.axis_index("cols")
    rows = count * size
    half = count // 2
    piece = half // parts
    vertices = rows * nz * nx * 2
    place = (z * nx + x) * 2 + k
    total = nz * nx * 2

    def row_device(index):
        index = lax.rem(index + total, total)
        return {
            "rows_0": lax.div(index, 2 * nx),
            "rows_1": lax.rem(lax.div(index, 2), nx),
            "rows_2": lax.rem(index, 2),
        }

    up, down = row_device(place + 1), row_device(place - 1)
    y_right, y_left = {"cols": lax.rem(y + 1, ny)}, {"cols": lax.rem(y + ny - 1, ny)}
    partner = {"rows_2": 1 - k}
    x_peers = [{"rows_1": lax.rem(x + d, nx)} for d in range(1, nx)]
    z_peers = [{"rows_0": lax.rem(z + d, nz)} for d in range(1, nz)]
    col_of = [y, lax.rem(y + ny - 1, ny), lax.rem(y + 1, ny), lax.rem(y + 2, ny)]

    load_basis = pltpu.make_async_copy(basis_ref, padded.at[pl.ds(BAND, count)], load_sem.at[0])
    load_basis.start()
    load_turn = []
    for i in range(ny):
        load = pltpu.make_async_copy(
            rot_ref.at[
                pl.ds(pl.multiple_of(col_of[i] * width, width), width),
                pl.ds(pl.multiple_of(y * width, width), width),
            ],
            turn.at[pl.ds(i * width, width)],
            load_sem.at[2 + i],
        )
        load.start()
        load_turn.append(load)
    load_blocks = pltpu.make_async_copy(blocks_ref, blocks, load_sem.at[1])
    load_blocks.start()

    peers = [up, down, y_right, y_left, partner, *x_peers, *z_peers]
    barrier = pltpu.get_barrier_semaphore()
    for peer in peers:
        pl.semaphore_signal(barrier, inc=1, device_id=peer, device_id_type=MESH)
    pl.semaphore_wait(barrier, len(peers))

    started = []

    def send(source, target, send_sem, recv_sem, device):
        copy = pltpu.make_async_remote_copy(
            src_ref=source,
            dst_ref=target,
            send_sem=send_sem,
            recv_sem=recv_sem,
            device_id=device,
            device_id_type=MESH,
        )
        copy.start()
        started.append(copy)
        return copy

    load_basis.wait()
    low, high = pl.ds(0, half), pl.ds(half, half)
    mine_low, mine_high = pl.ds(BAND, half), pl.ds(BAND + half, half)
    left_first = send(
        padded.at[mine_low], others.at[0, low], y_send.at[0], y_recv.at[0], y_right
    )
    right_first = send(
        padded.at[mine_high], others.at[1, high], y_send.at[1], y_recv.at[1], y_left
    )
    first_rows, last_rows = pl.ds(BAND, BAND), pl.ds(count, BAND)
    before, after = pl.ds(0, BAND), pl.ds(BAND + count, BAND)
    halo_low = send(
        padded.at[last_rows], padded.at[before], halo_send.at[0], halo_recv.at[0], up
    )
    halo_high = send(
        padded.at[first_rows], padded.at[after], halo_send.at[1], halo_recv.at[1], down
    )
    left_second = send(
        padded.at[mine_high], others.at[0, high], y_send.at[2], y_recv.at[2], y_right
    )
    right_second = send(
        padded.at[mine_low], others.at[1, low], y_send.at[3], y_recv.at[3], y_left
    )

    for b in range(count):
        at = pl.ds(b * size, size)
        column = jnp.broadcast_to(mass_ref[b : b + 1, :], (size, size)).T
        mass_col[at, :] = column
        own = padded[BAND + b].astype(F32)
        weights[at, width:] = (column * own).astype(BF16)

    def apply(source, store):
        for b in range(count):
            matrix = jnp.concatenate([blocks[b, n] for n in range(3)], axis=1)
            tiles = []
            for n in range(3):
                local = nb_ref[b, n] - place * count + BAND
                local = jnp.minimum(jnp.maximum(local, 0), count + 2 * BAND - 1)
                tiles.append(source[local])
            value = jnp.dot(
                matrix, jnp.concatenate(tiles, axis=0), preferred_element_type=F32
            )
            store(b, value)

    def store_image(b, value):
        weights[pl.ds(b * size, size), :width] = value.astype(BF16)

    load_blocks.wait()
    halo_low.wait_recv()
    halo_high.wait_recv()
    apply(padded, store_image)

    def add_gram(which, source, start, length, fresh):
        part = transposed_dot(source, weights[pl.ds(start * size, length * size), :])
        at = pl.ds(pl.multiple_of(col_of[which] * width, width), width)
        for j in range(2):
            value = part[:, j * width : (j + 1) * width]
            gram[j, at, :] = value if fresh else gram[j, at, :] + value

    def some(ref, start, length):
        return ref[pl.ds(start, length)].reshape(length * size, width)

    step = count // 4
    for i in range(4):
        add_gram(OWN, some(padded, BAND + i * step, step), i * step, step, i == 0)

    left_first.wait_recv()
    right_first.wait_recv()
    far_low, far_high = [], []
    for i in range(parts):
        at = pl.ds(i * piece, piece)
        far_low.append(
            send(
                others.at[0, at], others.at[2, at], y_send.at[4 + i], y_recv.at[4 + i], y_right
            )
        )
        at = pl.ds(half + i * piece, piece)
        j = 4 + parts + i
        far_high.append(
            send(others.at[1, at], others.at[2, at], y_send.at[j], y_recv.at[j], y_left)
        )
    left, right, far = (others.at[i] for i in range(3))
    for i in range(2):
        add_gram(LEFT, some(left, i * step, step), i * step, step, i == 0)
    for i in range(2, 4):
        add_gram(RIGHT, some(right, i * step, step), i * step, step, i == 2)
    for load in load_turn:
        load.wait()
    left_second.wait_recv()
    right_second.wait_recv()
    near = 3 * width
    for i in range(count // 2):
        joined = jnp.concatenate(
            [some(padded, BAND + 2 * i, 2), some(left, 2 * i, 2), some(right, 2 * i, 2)], axis=1
        )
        turned[pl.ds(2 * i * size, 2 * size), :] = jnp.dot(
            joined, turn[:near, :], preferred_element_type=F32
        )
    for i in range(2, 4):
        add_gram(LEFT, some(left, i * step, step), i * step, step, False)
    for i in range(2):
        add_gram(RIGHT, some(right, i * step, step), i * step, step, False)

    sums = jnp.zeros((8, width), F32)

    def far_turn(start, sums):
        at = pl.ds(start * size, piece * size)
        value = turned[at, :] + jnp.dot(
            some(far, start, piece), turn[near:, :], preferred_element_type=F32
        )
        turned[at, :] = value
        rimmed[pl.ds(BAND + start, piece)] = value.astype(BF16).reshape(piece, size, width)
        squares = mass_col[at, :] * value * value
        return sums + jnp.sum(squares.reshape(piece * size // 8, 8, width), axis=0)

    for i in range(parts):
        last = i == parts - 1
        far_low[i].wait_recv()
        far_high[i].wait_recv()
        for start in (i * piece, half + i * piece):
            sums = far_turn(start, sums)
        if last:
            sq_own[...] = jnp.sum(sums, axis=0, keepdims=True)
            sq_hop = send(sq_own, sq_core, core_send.at[1], core_recv.at[1], partner)
            rim_low = send(
                rimmed.at[last_rows], rimmed.at[before], halo_send.at[2], halo_recv.at[2], up
            )
            rim_high = send(
                rimmed.at[first_rows], rimmed.at[after], halo_send.at[3], halo_recv.at[3], down
            )
        for start in (i * piece, half + i * piece):
            add_gram(FAR, some(far, start, piece), start, piece, i == 0 and start == 0)

    gram_hop = send(gram.at[1 - k], gram_core, core_send.at[0], core_recv.at[0], partner)
    sq_hop.wait_recv()
    sq_x[...] = sq_own[...] + sq_core[...]
    sq_x_hops = [
        send(sq_x, sq_x_in.at[d], x_send.at[nx - 1 + d], x_recv.at[nx - 1 + d], peer)
        for d, peer in enumerate(x_peers)
    ]
    gram_hop.wait_recv()
    group = 8 * nx
    for i in range(nz):
        at = pl.ds(i * group, group)
        value = (gram[k, at, :] + gram_core[at, :]).reshape(nx, 8, width)
        for j in range(nx):
            gram_x[j, i] = value[j]
    gram_x_hops = [
        send(
            gram_x.at[lax.rem(x + 1 + d, nx)], gram_x_in.at[d], x_send.at[d], x_recv.at[d], peer
        )
        for d, peer in enumerate(x_peers)
    ]
    for hop in sq_x_hops:
        hop.wait_recv()
    value = sq_x[...]
    for d in range(nx - 1):
        value = value + sq_x_in[d]
    sq_z[...] = value
    sq_z_hops = [
        send(sq_z, sq_z_in.at[d], z_send.at[nz - 1 + d], z_recv.at[nz - 1 + d], peer)
        for d, peer in enumerate(z_peers)
    ]
    for hop in gram_x_hops:
        hop.wait_recv()
    value = gram_x[x]
    for d in range(nx - 1):
        value = value + gram_x_in[d]
    gram_z[...] = value
    gram_z_hops = [
        send(
            gram_z.at[lax.rem(z + 1 + d, nz)], gram_z_in.at[d], z_send.at[d], z_recv.at[d], peer
        )
        for d, peer in enumerate(z_peers)
    ]

    def store_product(b, value):
        product[pl.ds(b * size, size), :] = value

    rim_low.wait_recv()
    rim_high.wait_recv()
    apply(rimmed, store_product)

    for hop in sq_z_hops:
        hop.wait_recv()
    norm = sq_z[...]
    for d in range(nz - 1):
        norm = norm + sq_z_in[d]
    scale = lax.rsqrt(norm / vertices)

    for hop in gram_z_hops:
        hop.wait_recv()
    value = gram_z[z]
    for d in range(nz - 1):
        value = value + gram_z_in[d]
    tile_mine[...] = value / vertices
    tile_hop = send(tile_mine, tile_in, core_send.at[2], core_recv.at[2], partner)
    basis_out[...] = (turned[...] * scale).astype(BF16)
    image_out[...] = (product[...] * scale).astype(BF16)
    tile_hop.wait_recv()
    first = tile_mine[...]
    second = tile_in[...]
    stiff = jnp.where(k == 0, first, second)
    mass = jnp.where(k == 0, second, first)
    stiff_out[...] = jnp.where(k == 0, stiff[:4], stiff[4:])
    mass_out[...] = jnp.where(k == 0, mass[:4], mass[4:])
    for copy in started:
        copy.wait_send()


def body(basis_rows, stiff_blocks, block_neighbors, vertex_mass, rotation):
    nz, nx, _ = (lax.axis_size(a) for a in ROWS)
    ny = lax.axis_size("cols")
    rows, width = basis_rows.shape
    count, _, size, _ = stiff_blocks.shape
    parts = 2
    sizes = (nz, nx, ny, count, size, width, parts)
    reach = (count + 2 * BAND, size, width)
    vmem = pl.BlockSpec(memory_space=pltpu.VMEM)
    anywhere = pl.BlockSpec(memory_space=pl.ANY)
    dma = pltpu.SemaphoreType.DMA
    return pl.pallas_call(
        functools.partial(kernel, sizes),
        out_shape=(
            jax.ShapeDtypeStruct((rows, width), BF16),
            jax.ShapeDtypeStruct((rows, width), BF16),
            jax.ShapeDtypeStruct((4, width), F32),
            jax.ShapeDtypeStruct((4, width), F32),
        ),
        in_specs=[
            pl.BlockSpec(memory_space=pltpu.SMEM),
            anywhere,
            anywhere,
            vmem,
            anywhere,
        ],
        out_specs=(vmem, vmem, vmem, vmem),
        scratch_shapes=[
            pltpu.VMEM(reach, BF16),
            pltpu.VMEM((3, count, size, width), BF16),
            pltpu.VMEM(reach, BF16),
            pltpu.VMEM((rows, width), F32),
            pltpu.VMEM((rows, width), F32),
            pltpu.VMEM((rows, width), F32),
            pltpu.VMEM((rows, 2 * width), BF16),
            pltpu.VMEM(stiff_blocks.shape, BF16),
            pltpu.VMEM((ny * width, width), BF16),
            pltpu.VMEM((2, ny * width, width), F32),
            pltpu.VMEM((ny * width, width), F32),
            pltpu.VMEM((nx, nz, 8, width), F32),
            pltpu.VMEM((nx - 1, nz, 8, width), F32),
            pltpu.VMEM((nz, 8, width), F32),
            pltpu.VMEM((nz - 1, 8, width), F32),
            pltpu.VMEM((8, width), F32),
            pltpu.VMEM((8, width), F32),
            pltpu.VMEM((1, width), F32),
            pltpu.VMEM((1, width), F32),
            pltpu.VMEM((1, width), F32),
            pltpu.VMEM((nx - 1, 1, width), F32),
            pltpu.VMEM((1, width), F32),
            pltpu.VMEM((nz - 1, 1, width), F32),
            dma((2 + ny,)),
            dma((4 + 2 * parts,)),
            dma((4 + 2 * parts,)),
            dma((4,)),
            dma((4,)),
            dma((3,)),
            dma((3,)),
            dma((2 * (nx - 1),)),
            dma((2 * (nx - 1),)),
            dma((2 * (nz - 1),)),
            dma((2 * (nz - 1),)),
        ],
        compiler_params=pltpu.CompilerParams(collective_id=0, has_side_effects=True),
    )(
        block_neighbors,
        basis_rows.reshape(count, size, width),
        stiff_blocks,
        vertex_mass.reshape(count, size),
        rotation,
    )


def solution(mesh):
    split = Mesh(
        mesh.devices.reshape(16, 4, 2, mesh.shape["cols"]), ("rows_0", "rows_1", "rows_2", "cols")
    )
    in_specs = (P(ROWS, "cols"), P(ROWS, None, None, None), P(ROWS, None), P(ROWS), P())
    out_specs = (P(ROWS, "cols"), P(ROWS, "cols"), P(ROWS, "cols"), P(ROWS, "cols"))
    return jax.shard_map(body, mesh=split, in_specs=in_specs, out_specs=out_specs, check_vma=False)
```

```python
import functools

import jax
import jax.numpy as jnp
from jax import lax
from jax.experimental import pallas as pl
from jax.experimental.pallas import tpu as pltpu
from jax.sharding import Mesh
from jax.sharding import PartitionSpec as P

BAND = 8
ROWS = ("rows_0", "rows_1", "rows_2")
MESH = pl.DeviceIdType.MESH
F32 = jnp.float32
BF16 = jnp.bfloat16
LEFT, OWN, RIGHT, FAR = 0, 1, 2, 3
VMEM_LIMIT = 24 * 1024 * 1024
FINISH_LIMIT = 16 * 1024 * 1024


def transposed_dot(left, right):
    return lax.dot_general(left, right, (((0,), (0,)), ((), ())), preferred_element_type=F32)


def kernel(
    sizes,
    nb_ref,
    basis_ref,
    blocks_ref,
    mass_hbm,
    rot_ref,
    turned,
    product,
    scale_out,
    gram_out,
    padded,
    others,
    rimmed,
    mass_ref,
    mass_col,
    weights,
    blocks,
    turn,
    gram,
    plane,
    plane_in,
    line,
    line_in,
    sq_own,
    sq_plane_in,
    sq_line,
    sq_line_in,
    relay,
    load_sem,
    y_send,
    y_recv,
    halo_send,
    halo_recv,
    p_send,
    p_recv,
    z_send,
    z_recv,
):
    nz, nx, ny, count, size, width, parts = sizes
    z, x, k = (lax.axis_index(a) for a in ROWS)
    y = lax.axis_index("cols")
    half = count // 2
    piece = half // parts
    total = nz * nx * 2
    nq = 2 * nx
    q = 2 * x + k
    place = z * nq + q
    vertices = total * count * size
    slots = nz // ny
    early = nz - slots

    def row_device(index):
        index = lax.rem(index + total, total)
        return {
            "rows_0": lax.div(index, nq),
            "rows_1": lax.rem(lax.div(index, 2), nx),
            "rows_2": lax.rem(index, 2),
        }

    def along(axis, mine, length, step):
        return {axis: lax.rem(mine + length + step, length)}

    up, down = row_device(place + 1), row_device(place - 1)
    y_right, y_left = along("cols", y, ny, 1), along("cols", y, ny, -1)
    partner = {"rows_2": 1 - k}
    x_near = [along("rows_1", x, nx, d) for d in (1, -1)]
    z_near = [along("rows_0", z, nz, d) for d in (1, -1)]
    places = [lax.rem(q + d, nq) for d in range(1, nq)]
    q_peers = [{"rows_1": lax.div(p, 2), "rows_2": lax.rem(p, 2)} for p in places]
    z_peers = [along("rows_0", z, nz, d) for d in range(1, nz)]
    col_of = [lax.rem(y + ny - 1 + i, ny) for i in range(ny)]

    load_basis = pltpu.make_async_copy(basis_ref, padded.at[pl.ds(BAND, count)], load_sem.at[0])
    load_basis.start()
    load_mass = pltpu.make_async_copy(mass_hbm, mass_ref, load_sem.at[2 + ny])
    load_mass.start()

    peers = [y_right, y_left, partner, *x_near, *z_near]
    barrier = pltpu.get_barrier_semaphore()
    for peer in peers:
        pl.semaphore_signal(barrier, inc=1, device_id=peer, device_id_type=MESH)
    load_blocks = pltpu.make_async_copy(blocks_ref, blocks, load_sem.at[1])
    load_blocks.start()
    load_turn = []
    for i in range(ny):
        load = pltpu.make_async_copy(
            rot_ref.at[
                pl.ds(pl.multiple_of(col_of[i] * width, width), width),
                pl.ds(pl.multiple_of(y * width, width), width),
            ],
            turn.at[pl.ds(i * width, width)],
            load_sem.at[2 + i],
        )
        load.start()
        load_turn.append(load)
    load_basis.wait()
    pl.semaphore_wait(barrier, len(peers))

    started = []

    def send(source, target, send_sem, recv_sem, device):
        copy = pltpu.make_async_remote_copy(
            src_ref=source,
            dst_ref=target,
            send_sem=send_sem,
            recv_sem=recv_sem,
            device_id=device,
            device_id_type=MESH,
        )
        copy.start()
        started.append(copy)
        return copy

    low, high = pl.ds(0, half), pl.ds(half, half)
    mine_low, mine_high = pl.ds(BAND, half), pl.ds(BAND + half, half)
    left_first = send(
        padded.at[mine_low], others.at[0, low], y_send.at[0], y_recv.at[0], y_right
    )
    right_first = send(
        padded.at[mine_high], others.at[1, high], y_send.at[1], y_recv.at[1], y_left
    )
    left_second = send(
        padded.at[mine_high], others.at[0, high], y_send.at[2], y_recv.at[2], y_right
    )
    right_second = send(
        padded.at[mine_low], others.at[1, low], y_send.at[3], y_recv.at[3], y_left
    )

    relays = [
        [*z_near, *x_near, partner],
        [z_peers[1], z_peers[nz - 3], *x_near, partner],
        [z_peers[3], z_peers[nz - 5]],
    ]

    def tell(i):
        for peer in relays[i]:
            pl.semaphore_signal(relay.at[i], inc=1, device_id=peer, device_id_type=MESH)

    def hear(i):
        pl.semaphore_wait(relay.at[i], len(relays[i]))

    def weigh(b):
        at = pl.ds(b * size, size)
        column = jnp.broadcast_to(mass_ref[b : b + 1, :], (size, size)).T
        mass_col[at, :] = column
        weights[at, width:] = (column * padded[BAND + b].astype(F32)).astype(BF16)

    tell(0)
    load_mass.wait()
    for b in range(half):
        weigh(b)
    hear(0)
    tell(1)
    for b in range(half, count):
        weigh(b)
    hear(1)
    first_rows, last_rows = pl.ds(BAND, BAND), pl.ds(count, BAND)
    before, after = pl.ds(0, BAND), pl.ds(BAND + count, BAND)
    halo_low = send(
        padded.at[last_rows], padded.at[before], halo_send.at[0], halo_recv.at[0], up
    )
    halo_high = send(
        padded.at[first_rows], padded.at[after], halo_send.at[1], halo_recv.at[1], down
    )
    tell(2)

    def apply(source, store):
        for b in range(count):
            matrix = jnp.concatenate([blocks[b, n] for n in range(3)], axis=1)
            tiles = []
            for n in range(3):
                local = nb_ref[n, b] - place * count + BAND
                local = jnp.minimum(jnp.maximum(local, 0), count + 2 * BAND - 1)
                tiles.append(source[local])
            value = jnp.dot(
                matrix, jnp.concatenate(tiles, axis=0), preferred_element_type=F32
            )
            store(b, value)

    def store_image(b, value):
        weights[pl.ds(b * size, size), :width] = value.astype(BF16)

    load_blocks.wait()
    halo_low.wait_recv()
    halo_high.wait_recv()
    apply(padded, store_image)
    hear(2)

    def add_gram(which, source, start, length, fresh):
        part = transposed_dot(source, weights[pl.ds(start * size, length * size), :])
        for j in range(2):
            value = part[:, j * width : (j + 1) * width]
            gram[which, j] = value if fresh else gram[which, j] + value

    def some(ref, start, length):
        return ref[pl.ds(start, length)].reshape(length * size, width)

    step = count // 4
    for i in range(4):
        add_gram(OWN, some(padded, BAND + i * step, step), i * step, step, i == 0)

    left_first.wait_recv()
    right_first.wait_recv()
    chunks = []
    far_low, far_high = [], []
    for i in range(parts):
        starts = (i * piece, count - (i + 1) * piece)
        chunks.append(starts)
        at = pl.ds(starts[0], piece)
        j = 4 + i
        far_low.append(
            send(others.at[0, at], others.at[2, at], y_send.at[j], y_recv.at[j], y_right)
        )
        at = pl.ds(starts[1], piece)
        j = 4 + parts + i
        far_high.append(
            send(others.at[1, at], others.at[2, at], y_send.at[j], y_recv.at[j], y_left)
        )
    left, right, far = (others.at[i] for i in range(3))
    for i in range(2):
        add_gram(LEFT, some(left, i * step, step), i * step, step, i == 0)
    for i in range(2, 4):
        add_gram(RIGHT, some(right, i * step, step), i * step, step, i == 2)
    for load in load_turn:
        load.wait()
    left_second.wait_recv()
    right_second.wait_recv()
    for i in range(2, 4):
        add_gram(LEFT, some(left, i * step, step), i * step, step, False)
    for i in range(2):
        add_gram(RIGHT, some(right, i * step, step), i * step, step, False)

    def pack(which):
        for t in range(width // 8):
            for j in range(2):
                value = gram[which, j, pl.ds(8 * t, 8), :]
                at = slots * which + t // nx
                plane[2 * (t % nx), at, j] = value[:4]
                plane[2 * (t % nx) + 1, at, j] = value[4:]

    def plane_sends(at, offset):
        return [
            send(
                plane.at[places[d], at],
                plane_in.at[d, at],
                p_send.at[offset + d],
                p_recv.at[offset + d],
                peer,
            )
            for d, peer in enumerate(q_peers)
        ]

    def plane_sum(at):
        value = plane[q, at]
        for d in range(nq - 1):
            value = value + plane_in[d, at]
        line[at] = value

    for which in (LEFT, OWN, RIGHT):
        pack(which)
    early_at, late_at = pl.ds(0, early), pl.ds(early, slots)
    early_hops = plane_sends(early_at, 0)
    near = 3 * width
    for i in range(count // 2):
        joined = jnp.concatenate(
            [some(left, 2 * i, 2), some(padded, BAND + 2 * i, 2), some(right, 2 * i, 2)], axis=1
        )
        turned[pl.ds(2 * i * size, 2 * size), :] = jnp.dot(
            joined, turn[:near, :], preferred_element_type=F32
        )

    sums = jnp.zeros((8, width), F32)

    def far_turn(start, sums):
        at = pl.ds(start * size, piece * size)
        value = turned[at, :] + jnp.dot(
            some(far, start, piece), turn[near:, :], preferred_element_type=F32
        )
        turned[at, :] = value
        rimmed[pl.ds(BAND + start, piece)] = value.astype(BF16).reshape(piece, size, width)
        squares = mass_col[at, :] * value * value
        return sums + jnp.sum(squares.reshape(piece * size // 8, 8, width), axis=0)

    rims = []
    quarter = BAND // 2
    for i in range(parts):
        far_low[i].wait_recv()
        far_high[i].wait_recv()
        for start in chunks[i]:
            sums = far_turn(start, sums)
        if (i + 1) * piece % quarter == 0 and (i + 1) * piece <= BAND:
            done = (i + 1) * piece
            j = 2 + 2 * (done // quarter - 1)
            rims.append(
                send(
                    rimmed.at[pl.ds(BAND + done - quarter, quarter)],
                    rimmed.at[pl.ds(BAND + count + done - quarter, quarter)],
                    halo_send.at[j],
                    halo_recv.at[j],
                    down,
                )
            )
            rims.append(
                send(
                    rimmed.at[pl.ds(BAND + count - done, quarter)],
                    rimmed.at[pl.ds(BAND - done, quarter)],
                    halo_send.at[j + 1],
                    halo_recv.at[j + 1],
                    up,
                )
            )
        if i == parts - 2:
            for hop in early_hops:
                hop.wait_recv()
            plane_sum(early_at)
        if i == parts - 1:
            sq_own[...] = jnp.sum(sums, axis=0, keepdims=True)
            sq_hops = [
                send(
                    sq_own,
                    sq_plane_in.at[d],
                    p_send.at[2 * (nq - 1) + d],
                    p_recv.at[2 * (nq - 1) + d],
                    peer,
                )
                for d, peer in enumerate(q_peers)
            ]
        for j, start in enumerate(chunks[i]):
            add_gram(FAR, some(far, start, piece), start, piece, i == 0 and j == 0)

    pack(FAR)
    late_hops = plane_sends(late_at, nq - 1)
    for hop in sq_hops:
        hop.wait_recv()
    value = sq_own[...]
    for d in range(nq - 1):
        value = value + sq_plane_in[d]
    sq_line[...] = value
    sq_line_hops = [
        send(sq_line, sq_line_in.at[d], z_send.at[nz - 1 + d], z_recv.at[nz - 1 + d], peer)
        for d, peer in enumerate(z_peers)
    ]
    for hop in late_hops:
        hop.wait_recv()
    plane_sum(late_at)
    base = z + slots + nz - slots * y
    line_hops = [
        send(
            line.at[lax.rem(base + 1 + d, nz)], line_in.at[d], z_send.at[d], z_recv.at[d], peer
        )
        for d, peer in enumerate(z_peers)
    ]

    def store_product(b, value):
        product[pl.ds(b * size, size), :] = value

    for hop in rims:
        hop.wait_recv()
    apply(rimmed, store_product)

    for hop in sq_line_hops:
        hop.wait_recv()
    norm = sq_line[...]
    for d in range(nz - 1):
        norm = norm + sq_line_in[d]
    scale_out[...] = lax.rsqrt(norm / vertices)
    for hop in line_hops:
        hop.wait_recv()
    value = line[lax.rem(base, nz)]
    for d in range(nz - 1):
        value = value + line_in[d]
    gram_out[...] = value / vertices
    for copy in started:
        copy.wait_send()


def finish(
    turned, product, scale, gram, basis_out, image_out, stiff_out, mass_out, basis, image, sem
):
    rows = turned.shape[0]
    pieces = 4
    step = rows // pieces
    copies = []
    stiff_out[...] = gram[0]
    mass_out[...] = gram[1]
    for i in range(pieces):
        at = pl.ds(i * step, step)
        for j, (source, held, target) in enumerate(
            ((turned, basis, basis_out), (product, image, image_out))
        ):
            held[at, :] = (source[at, :] * scale[...]).astype(BF16)
            copy = pltpu.make_async_copy(held.at[at], target.at[at], sem.at[2 * i + j])
            copy.start()
            copies.append(copy)
    for copy in copies:
        copy.wait()


def in_hbm(value):
    return pltpu.with_memory_space_constraint(value, pltpu.HBM)


def body(basis_rows, stiff_blocks, block_neighbors, vertex_mass, rotation):
    nz, nx, _ = (lax.axis_size(a) for a in ROWS)
    ny = lax.axis_size("cols")
    rows, width = basis_rows.shape
    count, _, size, _ = stiff_blocks.shape
    parts = 5
    nq = 2 * nx
    sizes = (nz, nx, ny, count, size, width, parts)
    reach = (count + 2 * BAND, size, width)
    vmem = pl.BlockSpec(memory_space=pltpu.VMEM)
    hbm = pl.BlockSpec(memory_space=pltpu.HBM)
    dma = pltpu.SemaphoreType.DMA
    turned, product, scale, gram = pl.pallas_call(
        functools.partial(kernel, sizes),
        out_shape=(
            jax.ShapeDtypeStruct((rows, width), F32),
            jax.ShapeDtypeStruct((rows, width), F32),
            jax.ShapeDtypeStruct((1, width), F32),
            jax.ShapeDtypeStruct((2, 4, width), F32),
        ),
        in_specs=[pl.BlockSpec(memory_space=pltpu.SMEM), hbm, hbm, hbm, hbm],
        out_specs=(vmem, vmem, vmem, vmem),
        scratch_shapes=[
            pltpu.VMEM(reach, BF16),
            pltpu.VMEM((3, count, size, width), BF16),
            pltpu.VMEM(reach, BF16),
            pltpu.VMEM((count, size), F32),
            pltpu.VMEM((rows, width), F32),
            pltpu.VMEM((rows, 2 * width), BF16),
            pltpu.VMEM(stiff_blocks.shape, BF16),
            pltpu.VMEM((ny * width, width), BF16),
            pltpu.VMEM((ny, 2, width, width), F32),
            pltpu.VMEM((nq, nz, 2, 4, width), F32),
            pltpu.VMEM((nq - 1, nz, 2, 4, width), F32),
            pltpu.VMEM((nz, 2, 4, width), F32),
            pltpu.VMEM((nz - 1, 2, 4, width), F32),
            pltpu.VMEM((1, width), F32),
            pltpu.VMEM((nq - 1, 1, width), F32),
            pltpu.VMEM((1, width), F32),
            pltpu.VMEM((nz - 1, 1, width), F32),
            pltpu.SemaphoreType.REGULAR((3,)),
            dma((3 + ny,)),
            dma((4 + 2 * parts,)),
            dma((4 + 2 * parts,)),
            dma((6,)),
            dma((6,)),
            dma((3 * (nq - 1),)),
            dma((3 * (nq - 1),)),
            dma((2 * (nz - 1),)),
            dma((2 * (nz - 1),)),
        ],
        compiler_params=pltpu.CompilerParams(
            collective_id=0, has_side_effects=True, vmem_limit_bytes=VMEM_LIMIT
        ),
    )(
        in_hbm(block_neighbors.T),
        in_hbm(basis_rows.reshape(count, size, width)),
        in_hbm(stiff_blocks),
        in_hbm(vertex_mass.reshape(count, size)),
        in_hbm(rotation),
    )
    return pl.pallas_call(
        finish,
        out_shape=(
            jax.ShapeDtypeStruct((rows, width), BF16),
            jax.ShapeDtypeStruct((rows, width), BF16),
            jax.ShapeDtypeStruct((4, width), F32),
            jax.ShapeDtypeStruct((4, width), F32),
        ),
        in_specs=[vmem] * 4,
        out_specs=(hbm, hbm, vmem, vmem),
        scratch_shapes=[
            pltpu.VMEM((rows, width), BF16),
            pltpu.VMEM((rows, width), BF16),
            dma((8,)),
        ],
        compiler_params=pltpu.CompilerParams(vmem_limit_bytes=FINISH_LIMIT),
    )(turned, product, scale, gram)


def solution(mesh):
    split = Mesh(
        mesh.devices.reshape(16, 4, 2, mesh.shape["cols"]), ("rows_0", "rows_1", "rows_2", "cols")
    )
    in_specs = (P(ROWS, "cols"), P(ROWS, None, None, None), P(ROWS, None), P(ROWS), P())
    out_specs = (P(ROWS, "cols"), P(ROWS, "cols"), P(ROWS, "cols"), P(ROWS, "cols"))
    return jax.shard_map(body, mesh=split, in_specs=in_specs, out_specs=out_specs, check_vma=False)
```

```python
import functools

import jax
import jax.numpy as jnp
from jax import lax
from jax.experimental import pallas as pl
from jax.experimental.pallas import tpu as pltpu
from jax.sharding import Mesh
from jax.sharding import PartitionSpec as P

BAND = 8
ROWS = ("rows_0", "rows_1", "rows_2")
MESH = pl.DeviceIdType.MESH
F32 = jnp.float32
BF16 = jnp.bfloat16
LEFT, OWN, RIGHT, FAR = 0, 1, 2, 3
VMEM_LIMIT = 24 * 1024 * 1024
FINISH_LIMIT = 16 * 1024 * 1024


def transposed_dot(left, right):
    return lax.dot_general(left, right, (((0,), (0,)), ((), ())), preferred_element_type=F32)


def kernel(
    sizes,
    nb_ref,
    basis_ref,
    blocks_ref,
    mass_hbm,
    rot_ref,
    turned,
    product,
    scale_out,
    gram_out,
    padded,
    others,
    rimmed,
    mass_ref,
    mass_col,
    weights,
    blocks,
    turn,
    gram,
    plane,
    plane_in,
    line,
    line_in,
    sq_own,
    sq_plane_in,
    sq_line,
    sq_line_in,
    relay,
    load_sem,
    y_send,
    y_recv,
    halo_send,
    halo_recv,
    p_send,
    p_recv,
    z_send,
    z_recv,
):
    nz, nx, ny, count, size, width, parts = sizes
    z, x, k = (lax.axis_index(a) for a in ROWS)
    y = lax.axis_index("cols")
    half = count // 2
    piece = half // parts
    total = nz * nx * 2
    nq = 2 * nx
    q = 2 * x + k
    place = z * nq + q
    vertices = total * count * size
    slots = nz // ny
    early = nz - slots

    def row_device(index):
        index = lax.rem(index + total, total)
        return {
            "rows_0": lax.div(index, nq),
            "rows_1": lax.rem(lax.div(index, 2), nx),
            "rows_2": lax.rem(index, 2),
        }

    def along(axis, mine, length, step):
        return {axis: lax.rem(mine + length + step, length)}

    up, down = row_device(place + 1), row_device(place - 1)
    y_right, y_left = along("cols", y, ny, 1), along("cols", y, ny, -1)
    partner = {"rows_2": 1 - k}
    x_near = [along("rows_1", x, nx, d) for d in (1, -1)]
    z_near = [along("rows_0", z, nz, d) for d in (1, -1)]
    places = [lax.rem(q + d, nq) for d in range(1, nq)]
    q_peers = [{"rows_1": lax.div(p, 2), "rows_2": lax.rem(p, 2)} for p in places]
    z_peers = [along("rows_0", z, nz, d) for d in range(1, nz)]
    col_of = [lax.rem(y + ny - 1 + i, ny) for i in range(ny)]

    load_basis = pltpu.make_async_copy(basis_ref, padded.at[pl.ds(BAND, count)], load_sem.at[0])
    load_basis.start()
    load_mass = pltpu.make_async_copy(mass_hbm, mass_ref, load_sem.at[3 + ny])
    load_mass.start()

    peers = [y_right, y_left, partner, *x_near, *z_near]
    barrier = pltpu.get_barrier_semaphore()
    for peer in peers:
        pl.semaphore_signal(barrier, inc=1, device_id=peer, device_id_type=MESH)
    load_blocks = pltpu.make_async_copy(blocks_ref, blocks, load_sem.at[1])
    load_blocks.start()
    load_turn = []
    for i in range(ny + 1):
        load = pltpu.make_async_copy(
            rot_ref.at[
                pl.ds(pl.multiple_of(col_of[i % ny] * width, width), width),
                pl.ds(pl.multiple_of(y * width, width), width),
            ],
            turn.at[pl.ds(i * width, width)],
            load_sem.at[2 + i],
        )
        load.start()
        load_turn.append(load)
    load_basis.wait()
    pl.semaphore_wait(barrier, len(peers))

    started = []

    def send(source, target, send_sem, recv_sem, device):
        copy = pltpu.make_async_remote_copy(
            src_ref=source,
            dst_ref=target,
            send_sem=send_sem,
            recv_sem=recv_sem,
            device_id=device,
            device_id_type=MESH,
        )
        copy.start()
        started.append(copy)
        return copy

    low, high = pl.ds(0, half), pl.ds(half, half)
    mine_low, mine_high = pl.ds(BAND, half), pl.ds(BAND + half, half)
    left_first = send(
        padded.at[mine_low], others.at[0, low], y_send.at[0], y_recv.at[0], y_right
    )
    right_first = send(
        padded.at[mine_high], others.at[1, high], y_send.at[1], y_recv.at[1], y_left
    )
    left_second = send(
        padded.at[mine_high], others.at[0, high], y_send.at[2], y_recv.at[2], y_right
    )
    right_second = send(
        padded.at[mine_low], others.at[1, low], y_send.at[3], y_recv.at[3], y_left
    )

    relays = [
        [*z_near, *x_near, partner],
        [z_peers[1], z_peers[nz - 3], *x_near, partner],
        [z_peers[3], z_peers[nz - 5]],
    ]

    def tell(i):
        for peer in relays[i]:
            pl.semaphore_signal(relay.at[i], inc=1, device_id=peer, device_id_type=MESH)

    def hear(i):
        pl.semaphore_wait(relay.at[i], len(relays[i]))

    def weigh(b):
        at = pl.ds(b * size, size)
        column = jnp.broadcast_to(mass_ref[b : b + 1, :], (size, size)).T
        mass_col[at, :] = column
        weights[at, width:] = (column * padded[BAND + b].astype(F32)).astype(BF16)

    tell(0)
    load_mass.wait()
    for b in range(half):
        weigh(b)
    hear(0)
    tell(1)
    for b in range(half, count):
        weigh(b)
    hear(1)
    first_rows, last_rows = pl.ds(BAND, BAND), pl.ds(count, BAND)
    before, after = pl.ds(0, BAND), pl.ds(BAND + count, BAND)
    halo_low = send(
        padded.at[last_rows], padded.at[before], halo_send.at[0], halo_recv.at[0], up
    )
    halo_high = send(
        padded.at[first_rows], padded.at[after], halo_send.at[1], halo_recv.at[1], down
    )
    tell(2)

    def apply(source, store):
        for b in range(count):
            matrix = jnp.concatenate([blocks[b, n] for n in range(3)], axis=1)
            tiles = []
            for n in range(3):
                local = nb_ref[n, b] - place * count + BAND
                local = jnp.minimum(jnp.maximum(local, 0), count + 2 * BAND - 1)
                tiles.append(source[local])
            value = jnp.dot(
                matrix, jnp.concatenate(tiles, axis=0), preferred_element_type=F32
            )
            store(b, value)

    def store_image(b, value):
        weights[pl.ds(b * size, size), :width] = value.astype(BF16)

    load_blocks.wait()
    halo_low.wait_recv()
    halo_high.wait_recv()
    apply(padded, store_image)
    hear(2)

    def add_gram(which, source, start, length, fresh):
        part = transposed_dot(source, weights[pl.ds(start * size, length * size), :])
        for j in range(2):
            value = part[:, j * width : (j + 1) * width]
            gram[which, j] = value if fresh else gram[which, j] + value

    def some(ref, start, length):
        return ref[pl.ds(start, length)].reshape(length * size, width)

    step = count // 4
    for i in range(4):
        add_gram(OWN, some(padded, BAND + i * step, step), i * step, step, i == 0)

    def pack(which):
        for t in range(width // 8):
            for j in range(2):
                value = gram[which, j, pl.ds(8 * t, 8), :]
                at = slots * which + t // nx
                plane[2 * (t % nx), at, j] = value[:4]
                plane[2 * (t % nx) + 1, at, j] = value[4:]

    def plane_sends(at, offset):
        return [
            send(
                plane.at[places[d], at],
                plane_in.at[d, at],
                p_send.at[offset + d],
                p_recv.at[offset + d],
                peer,
            )
            for d, peer in enumerate(q_peers)
        ]

    def plane_sum(at):
        value = plane[q, at]
        for d in range(nq - 1):
            value = value + plane_in[d, at]
        line[at] = value

    at_piece = [pl.ds(slots * i, slots) for i in range(ny)]
    pack(OWN)
    early_hops = plane_sends(at_piece[OWN], 0)

    left_first.wait_recv()
    right_first.wait_recv()
    chunks = []
    far_low, far_high = [], []
    for i in range(parts):
        starts = (i * piece, count - (i + 1) * piece)
        chunks.append(starts)
        at = pl.ds(starts[0], piece)
        j = 4 + i
        far_low.append(
            send(others.at[0, at], others.at[2, at], y_send.at[j], y_recv.at[j], y_right)
        )
        at = pl.ds(starts[1], piece)
        j = 4 + parts + i
        far_high.append(
            send(others.at[1, at], others.at[2, at], y_send.at[j], y_recv.at[j], y_left)
        )
    left, right, far = (others.at[i] for i in range(3))
    for i in range(2):
        add_gram(LEFT, some(left, i * step, step), i * step, step, i == 0)
    for i in range(2, 4):
        add_gram(RIGHT, some(right, i * step, step), i * step, step, i == 2)
    for load in load_turn:
        load.wait()
    for i in range(count // 2):
        own = some(padded, BAND + 2 * i, 2)
        if 2 * i < half:
            pair, at = [some(left, 2 * i, 2), own], pl.ds(0, 2 * width)
        else:
            pair, at = [own, some(right, 2 * i, 2)], pl.ds(width, 2 * width)
        turned[pl.ds(2 * i * size, 2 * size), :] = jnp.dot(
            jnp.concatenate(pair, axis=1), turn[at, :], preferred_element_type=F32
        )
    left_second.wait_recv()
    right_second.wait_recv()
    for i in range(2, 4):
        add_gram(LEFT, some(left, i * step, step), i * step, step, False)
    for i in range(2):
        add_gram(RIGHT, some(right, i * step, step), i * step, step, False)

    pack(LEFT)
    early_hops += plane_sends(at_piece[LEFT], nq - 1)
    pack(RIGHT)
    early_hops += plane_sends(at_piece[RIGHT], 2 * (nq - 1))

    sums = jnp.zeros((8, width), F32)

    def far_turn(start, sums):
        at = pl.ds(start * size, piece * size)
        if start < half:
            pair, place_of = [some(right, start, piece), some(far, start, piece)], 2
        else:
            pair, place_of = [some(far, start, piece), some(left, start, piece)], 3
        value = turned[at, :] + jnp.dot(
            jnp.concatenate(pair, axis=1),
            turn[pl.ds(place_of * width, 2 * width), :],
            preferred_element_type=F32,
        )
        turned[at, :] = value
        rimmed[pl.ds(BAND + start, piece)] = value.astype(BF16).reshape(piece, size, width)
        squares = mass_col[at, :] * value * value
        return sums + jnp.sum(squares.reshape(piece * size // 8, 8, width), axis=0)

    rims = []
    quarter = BAND // 2
    def send_rims(done):
        j = 2 + 2 * (done // quarter - 1)
        rims.append(
            send(
                rimmed.at[pl.ds(BAND + done - quarter, quarter)],
                rimmed.at[pl.ds(BAND + count + done - quarter, quarter)],
                halo_send.at[j],
                halo_recv.at[j],
                down,
            )
        )
        rims.append(
            send(
                rimmed.at[pl.ds(BAND + count - done, quarter)],
                rimmed.at[pl.ds(BAND - done, quarter)],
                halo_send.at[j + 1],
                halo_recv.at[j + 1],
                up,
            )
        )

    def far_gram(i):
        for j, start in enumerate(chunks[i]):
            add_gram(FAR, some(far, start, piece), start, piece, i == 0 and j == 0)

    slot_of = [lax.rem(z + d + slots + nz - slots * y, nz) for d in range(nz)]
    line_copies = [
        pltpu.make_async_remote_copy(
            src_ref=line.at[slot_of[d + 1]],
            dst_ref=line_in.at[d],
            send_sem=z_send.at[d],
            recv_sem=z_recv.at[d],
            device_id=peer,
            device_id_type=MESH,
        )
        for d, peer in enumerate(z_peers)
    ]
    far_first = sorted(range(nz - 1), key=lambda d: abs(d + 1 - nz // 2))

    for i in range(parts - 1):
        far_low[i].wait_recv()
        far_high[i].wait_recv()
        for start in chunks[i]:
            sums = far_turn(start, sums)
        if (i + 1) * piece % quarter == 0 and (i + 1) * piece <= BAND:
            send_rims((i + 1) * piece)
        far_gram(i)
    early_at, late_at = pl.ds(0, early), pl.ds(early, slots)
    for hop in early_hops:
        hop.wait_recv()
    plane_sum(early_at)
    for d in far_first:
        pl.when(slot_of[d + 1] < early)(line_copies[d].start)
    last = parts - 1
    far_low[last].wait_recv()
    far_high[last].wait_recv()
    far_gram(last)
    pack(FAR)
    late_hops = plane_sends(late_at, 3 * (nq - 1))
    for start in chunks[last]:
        sums = far_turn(start, sums)
    sq_own[...] = jnp.sum(sums, axis=0, keepdims=True)
    sq_hops = [
        send(
            sq_own,
            sq_plane_in.at[d],
            p_send.at[4 * (nq - 1) + d],
            p_recv.at[4 * (nq - 1) + d],
            peer,
        )
        for d, peer in enumerate(q_peers)
    ]
    for hop in late_hops:
        hop.wait_recv()
    plane_sum(late_at)
    for d in far_first:
        pl.when(slot_of[d + 1] >= early)(line_copies[d].start)
    for hop in sq_hops:
        hop.wait_recv()
    value = sq_own[...]
    for d in range(nq - 1):
        value = value + sq_plane_in[d]
    sq_line[...] = value
    sq_line_hops = [
        send(sq_line, sq_line_in.at[d], z_send.at[nz - 1 + d], z_recv.at[nz - 1 + d], peer)
        for d, peer in enumerate(z_peers)
    ]
    def store_product(b, value):
        product[pl.ds(b * size, size), :] = value

    for hop in rims:
        hop.wait_recv()
    apply(rimmed, store_product)

    for hop in sq_line_hops:
        hop.wait_recv()
    norm = sq_line[...]
    for d in range(nz - 1):
        norm = norm + sq_line_in[d]
    scale_out[...] = lax.rsqrt(norm / vertices)
    for copy in line_copies:
        copy.wait_recv()
    value = line[slot_of[0]]
    for d in range(nz - 1):
        value = value + line_in[d]
    gram_out[...] = value / vertices
    for copy in started + line_copies:
        copy.wait_send()


def finish(
    turned, product, scale, gram, basis_out, image_out, stiff_out, mass_out, basis, image, sem
):
    rows = turned.shape[0]
    pieces = 4
    step = rows // pieces
    copies = []
    stiff_out[...] = gram[0]
    mass_out[...] = gram[1]
    for i in range(pieces):
        at = pl.ds(i * step, step)
        for j, (source, held, target) in enumerate(
            ((turned, basis, basis_out), (product, image, image_out))
        ):
            held[at, :] = (source[at, :] * scale[...]).astype(BF16)
            copy = pltpu.make_async_copy(held.at[at], target.at[at], sem.at[2 * i + j])
            copy.start()
            copies.append(copy)
    for copy in copies:
        copy.wait()


def in_hbm(value):
    return pltpu.with_memory_space_constraint(value, pltpu.HBM)


def body(basis_rows, stiff_blocks, block_neighbors, vertex_mass, rotation):
    nz, nx, _ = (lax.axis_size(a) for a in ROWS)
    ny = lax.axis_size("cols")
    rows, width = basis_rows.shape
    count, _, size, _ = stiff_blocks.shape
    parts = 5
    nq = 2 * nx
    sizes = (nz, nx, ny, count, size, width, parts)
    reach = (count + 2 * BAND, size, width)
    vmem = pl.BlockSpec(memory_space=pltpu.VMEM)
    hbm = pl.BlockSpec(memory_space=pltpu.HBM)
    dma = pltpu.SemaphoreType.DMA
    turned, product, scale, gram = pl.pallas_call(
        functools.partial(kernel, sizes),
        out_shape=(
            jax.ShapeDtypeStruct((rows, width), F32),
            jax.ShapeDtypeStruct((rows, width), F32),
            jax.ShapeDtypeStruct((1, width), F32),
            jax.ShapeDtypeStruct((2, 4, width), F32),
        ),
        in_specs=[pl.BlockSpec(memory_space=pltpu.SMEM), hbm, hbm, hbm, hbm],
        out_specs=(vmem, vmem, vmem, vmem),
        scratch_shapes=[
            pltpu.VMEM(reach, BF16),
            pltpu.VMEM((3, count, size, width), BF16),
            pltpu.VMEM(reach, BF16),
            pltpu.VMEM((count, size), F32),
            pltpu.VMEM((rows, width), F32),
            pltpu.VMEM((rows, 2 * width), BF16),
            pltpu.VMEM(stiff_blocks.shape, BF16),
            pltpu.VMEM(((ny + 1) * width, width), BF16),
            pltpu.VMEM((ny, 2, width, width), F32),
            pltpu.VMEM((nq, nz, 2, 4, width), F32),
            pltpu.VMEM((nq - 1, nz, 2, 4, width), F32),
            pltpu.VMEM((nz, 2, 4, width), F32),
            pltpu.VMEM((nz - 1, 2, 4, width), F32),
            pltpu.VMEM((1, width), F32),
            pltpu.VMEM((nq - 1, 1, width), F32),
            pltpu.VMEM((1, width), F32),
            pltpu.VMEM((nz - 1, 1, width), F32),
            pltpu.SemaphoreType.REGULAR((3,)),
            dma((4 + ny,)),
            dma((4 + 2 * parts,)),
            dma((4 + 2 * parts,)),
            dma((6,)),
            dma((6,)),
            dma((5 * (nq - 1),)),
            dma((5 * (nq - 1),)),
            dma((2 * (nz - 1),)),
            dma((2 * (nz - 1),)),
        ],
        compiler_params=pltpu.CompilerParams(
            collective_id=0, has_side_effects=True, vmem_limit_bytes=VMEM_LIMIT
        ),
    )(
        in_hbm(block_neighbors.T),
        in_hbm(basis_rows.reshape(count, size, width)),
        in_hbm(stiff_blocks),
        in_hbm(vertex_mass.reshape(count, size)),
        in_hbm(rotation),
    )
    return pl.pallas_call(
        finish,
        out_shape=(
            jax.ShapeDtypeStruct((rows, width), BF16),
            jax.ShapeDtypeStruct((rows, width), BF16),
            jax.ShapeDtypeStruct((4, width), F32),
            jax.ShapeDtypeStruct((4, width), F32),
        ),
        in_specs=[vmem] * 4,
        out_specs=(hbm, hbm, vmem, vmem),
        scratch_shapes=[
            pltpu.VMEM((rows, width), BF16),
            pltpu.VMEM((rows, width), BF16),
            dma((8,)),
        ],
        compiler_params=pltpu.CompilerParams(vmem_limit_bytes=FINISH_LIMIT),
    )(turned, product, scale, gram)


def solution(mesh):
    split = Mesh(
        mesh.devices.reshape(16, 4, 2, mesh.shape["cols"]), ("rows_0", "rows_1", "rows_2", "cols")
    )
    in_specs = (P(ROWS, "cols"), P(ROWS, None, None, None), P(ROWS, None), P(ROWS), P())
    out_specs = (P(ROWS, "cols"), P(ROWS, "cols"), P(ROWS, "cols"), P(ROWS, "cols"))
    return jax.shard_map(body, mesh=split, in_specs=in_specs, out_specs=out_specs, check_vma=False)
```

```python
import functools

import jax
import jax.numpy as jnp
from jax import lax
from jax.experimental import pallas as pl
from jax.experimental.pallas import tpu as pltpu
from jax.sharding import Mesh
from jax.sharding import PartitionSpec as P

BAND = 8
ROWS = ("rows_0", "rows_1", "rows_2")
MESH = pl.DeviceIdType.MESH
F32 = jnp.float32
BF16 = jnp.bfloat16
LEFT, OWN, RIGHT, FAR = 0, 1, 2, 3
VMEM_LIMIT = 24 * 1024 * 1024
FINISH_LIMIT = 16 * 1024 * 1024


def transposed_dot(left, right):
    return lax.dot_general(left, right, (((0,), (0,)), ((), ())), preferred_element_type=F32)


def kernel(
    sizes,
    nb_hbm,
    basis_ref,
    blocks_ref,
    mass_hbm,
    rot_ref,
    turned,
    product,
    scale_out,
    gram_out,
    padded,
    others,
    rimmed,
    nb_ref,
    mass_ref,
    mass_col,
    weights,
    blocks,
    turn,
    gram,
    plane,
    plane_in,
    line,
    line_in,
    sq_own,
    sq_plane_in,
    sq_line,
    sq_line_in,
    relay,
    load_sem,
    y_send,
    y_recv,
    halo_send,
    halo_recv,
    p_send,
    p_recv,
    z_send,
    z_recv,
):
    nz, nx, ny, count, size, width, pieces = sizes
    z, x, k = (lax.axis_index(a) for a in ROWS)
    y = lax.axis_index("cols")
    half = count // 2
    parts = len(pieces)
    begins = [sum(pieces[:i]) for i in range(parts)]
    total = nz * nx * 2
    nq = 2 * nx
    q = 2 * x + k
    place = z * nq + q
    vertices = total * count * size
    slots = nz // ny
    early = nz - slots

    def row_device(index):
        index = lax.rem(index + total, total)
        return {
            "rows_0": lax.div(index, nq),
            "rows_1": lax.rem(lax.div(index, 2), nx),
            "rows_2": lax.rem(index, 2),
        }

    def along(axis, mine, length, step):
        return {axis: lax.rem(mine + length + step, length)}

    up, down = row_device(place + 1), row_device(place - 1)
    y_right, y_left = along("cols", y, ny, 1), along("cols", y, ny, -1)
    partner = {"rows_2": 1 - k}
    x_near = [along("rows_1", x, nx, d) for d in (1, -1)]
    z_near = [along("rows_0", z, nz, d) for d in (1, -1)]
    places = [lax.rem(q + d, nq) for d in range(1, nq)]
    q_peers = [{"rows_1": lax.div(p, 2), "rows_2": lax.rem(p, 2)} for p in places]
    z_peers = [along("rows_0", z, nz, d) for d in range(1, nz)]
    col_of = [lax.rem(y + ny - 1 + i, ny) for i in range(ny)]

    load_basis = pltpu.make_async_copy(basis_ref, padded.at[pl.ds(BAND, count)], load_sem.at[0])
    load_basis.start()
    load_mass = pltpu.make_async_copy(mass_hbm, mass_ref, load_sem.at[3 + ny])
    load_mass.start()
    load_nb = pltpu.make_async_copy(nb_hbm, nb_ref, load_sem.at[4 + ny])
    load_nb.start()

    peers = [y_right, y_left, partner, *x_near, *z_near]
    barrier = pltpu.get_barrier_semaphore()
    for peer in peers:
        pl.semaphore_signal(barrier, inc=1, device_id=peer, device_id_type=MESH)
    load_blocks = pltpu.make_async_copy(blocks_ref, blocks, load_sem.at[1])
    load_blocks.start()
    load_turn = []
    for i in range(ny + 1):
        load = pltpu.make_async_copy(
            rot_ref.at[
                pl.ds(pl.multiple_of(col_of[i % ny] * width, width), width),
                pl.ds(pl.multiple_of(y * width, width), width),
            ],
            turn.at[pl.ds(i * width, width)],
            load_sem.at[2 + i],
        )
        load.start()
        load_turn.append(load)
    load_basis.wait()
    pl.semaphore_wait(barrier, len(peers))

    started = []

    def send(source, target, send_sem, recv_sem, device):
        copy = pltpu.make_async_remote_copy(
            src_ref=source,
            dst_ref=target,
            send_sem=send_sem,
            recv_sem=recv_sem,
            device_id=device,
            device_id_type=MESH,
        )
        copy.start()
        started.append(copy)
        return copy

    low, high = pl.ds(0, half), pl.ds(half, half)
    mine_low, mine_high = pl.ds(BAND, half), pl.ds(BAND + half, half)
    left_first = send(
        padded.at[mine_low], others.at[0, low], y_send.at[0], y_recv.at[0], y_right
    )
    right_first = send(
        padded.at[mine_high], others.at[1, high], y_send.at[1], y_recv.at[1], y_left
    )
    left_second = send(
        padded.at[mine_high], others.at[0, high], y_send.at[2], y_recv.at[2], y_right
    )
    right_second = send(
        padded.at[mine_low], others.at[1, low], y_send.at[3], y_recv.at[3], y_left
    )

    relays = [
        [*z_near, *x_near, partner],
        [z_peers[1], z_peers[nz - 3], *x_near, partner],
        [z_peers[3], z_peers[nz - 5]],
    ]

    def tell(i):
        for peer in relays[i]:
            pl.semaphore_signal(relay.at[i], inc=1, device_id=peer, device_id_type=MESH)

    def hear(i):
        pl.semaphore_wait(relay.at[i], len(relays[i]))

    def weigh(b):
        at = pl.ds(b * size, size)
        column = jnp.broadcast_to(mass_ref[b : b + 1, :], (size, size)).T
        mass_col[at, :] = column
        weights[at, width:] = (column * padded[BAND + b].astype(F32)).astype(BF16)

    tell(0)
    load_mass.wait()
    for b in range(half):
        weigh(b)
    hear(0)
    tell(1)
    for b in range(half, count):
        weigh(b)
    hear(1)
    first_rows, last_rows = pl.ds(BAND, BAND), pl.ds(count, BAND)
    before, after = pl.ds(0, BAND), pl.ds(BAND + count, BAND)
    halo_low = send(
        padded.at[last_rows], padded.at[before], halo_send.at[0], halo_recv.at[0], up
    )
    halo_high = send(
        padded.at[first_rows], padded.at[after], halo_send.at[1], halo_recv.at[1], down
    )
    tell(2)

    def apply(source, store):
        for b in range(count):
            matrix = jnp.concatenate([blocks[b, n] for n in range(3)], axis=1)
            tiles = []
            for n in range(3):
                local = nb_ref[n, b] - place * count + BAND
                local = jnp.minimum(jnp.maximum(local, 0), count + 2 * BAND - 1)
                tiles.append(source[local])
            value = jnp.dot(
                matrix, jnp.concatenate(tiles, axis=0), preferred_element_type=F32
            )
            store(b, value)

    def store_image(b, value):
        weights[pl.ds(b * size, size), :width] = value.astype(BF16)

    load_blocks.wait()
    load_nb.wait()
    halo_low.wait_recv()
    halo_high.wait_recv()
    apply(padded, store_image)
    hear(2)

    def add_gram(which, source, start, length, fresh):
        part = transposed_dot(source, weights[pl.ds(start * size, length * size), :])
        for j in range(2):
            value = part[:, j * width : (j + 1) * width]
            gram[which, j] = value if fresh else gram[which, j] + value

    def some(ref, start, length):
        return ref[pl.ds(start, length)].reshape(length * size, width)

    step = count // 4
    for i in range(4):
        add_gram(OWN, some(padded, BAND + i * step, step), i * step, step, i == 0)

    def pack(which):
        for t in range(width // 8):
            for j in range(2):
                value = gram[which, j, pl.ds(8 * t, 8), :]
                at = slots * which + t // nx
                plane[2 * (t % nx), at, j] = value[:4]
                plane[2 * (t % nx) + 1, at, j] = value[4:]

    def plane_sends(at, offset):
        return [
            send(
                plane.at[places[d], at],
                plane_in.at[d, at],
                p_send.at[offset + d],
                p_recv.at[offset + d],
                peer,
            )
            for d, peer in enumerate(q_peers)
        ]

    def plane_sum(at):
        value = plane[q, at]
        for d in range(nq - 1):
            value = value + plane_in[d, at]
        line[at] = value

    at_piece = [pl.ds(slots * i, slots) for i in range(ny)]
    pack(OWN)
    early_hops = plane_sends(at_piece[OWN], 0)

    left_first.wait_recv()
    right_first.wait_recv()
    chunks = []
    far_low, far_high = [], []
    for i in range(parts):
        starts = (begins[i], count - begins[i] - pieces[i])
        chunks.append(starts)
        at = pl.ds(starts[0], pieces[i])
        j = 4 + i
        far_low.append(
            send(others.at[0, at], others.at[2, at], y_send.at[j], y_recv.at[j], y_right)
        )
        at = pl.ds(starts[1], pieces[i])
        j = 4 + parts + i
        far_high.append(
            send(others.at[1, at], others.at[2, at], y_send.at[j], y_recv.at[j], y_left)
        )
    left, right, far = (others.at[i] for i in range(3))
    for i in range(2):
        add_gram(LEFT, some(left, i * step, step), i * step, step, i == 0)
    for i in range(2, 4):
        add_gram(RIGHT, some(right, i * step, step), i * step, step, i == 2)
    for load in load_turn:
        load.wait()
    for i in range(count // 2):
        own = some(padded, BAND + 2 * i, 2)
        if 2 * i < half:
            pair, at = [some(left, 2 * i, 2), own], pl.ds(0, 2 * width)
        else:
            pair, at = [own, some(right, 2 * i, 2)], pl.ds(width, 2 * width)
        turned[pl.ds(2 * i * size, 2 * size), :] = jnp.dot(
            jnp.concatenate(pair, axis=1), turn[at, :], preferred_element_type=F32
        )
    left_second.wait_recv()
    right_second.wait_recv()
    for i in range(2, 4):
        add_gram(LEFT, some(left, i * step, step), i * step, step, False)
    for i in range(2):
        add_gram(RIGHT, some(right, i * step, step), i * step, step, False)

    pack(LEFT)
    early_hops += plane_sends(at_piece[LEFT], nq - 1)
    pack(RIGHT)
    early_hops += plane_sends(at_piece[RIGHT], 2 * (nq - 1))

    sums = jnp.zeros((8, width), F32)

    def far_turn(start, piece, sums):
        at = pl.ds(start * size, piece * size)
        if start < half:
            pair, place_of = [some(right, start, piece), some(far, start, piece)], 2
        else:
            pair, place_of = [some(far, start, piece), some(left, start, piece)], 3
        value = turned[at, :] + jnp.dot(
            jnp.concatenate(pair, axis=1),
            turn[pl.ds(place_of * width, 2 * width), :],
            preferred_element_type=F32,
        )
        turned[at, :] = value
        rimmed[pl.ds(BAND + start, piece)] = value.astype(BF16).reshape(piece, size, width)
        squares = mass_col[at, :] * value * value
        return sums + jnp.sum(squares.reshape(piece * size // 8, 8, width), axis=0)

    rims = []
    quarter = BAND // 2
    def send_rims(done):
        j = 2 + 2 * (done // quarter - 1)
        rims.append(
            send(
                rimmed.at[pl.ds(BAND + done - quarter, quarter)],
                rimmed.at[pl.ds(BAND + count + done - quarter, quarter)],
                halo_send.at[j],
                halo_recv.at[j],
                down,
            )
        )
        rims.append(
            send(
                rimmed.at[pl.ds(BAND + count - done, quarter)],
                rimmed.at[pl.ds(BAND - done, quarter)],
                halo_send.at[j + 1],
                halo_recv.at[j + 1],
                up,
            )
        )

    def far_gram(i):
        for j, start in enumerate(chunks[i]):
            source = some(far, start, pieces[i])
            add_gram(FAR, source, start, pieces[i], i == 0 and j == 0)

    slot_of = [lax.rem(z + d + slots + nz - slots * y, nz) for d in range(nz)]
    line_copies = [
        pltpu.make_async_remote_copy(
            src_ref=line.at[slot_of[d + 1]],
            dst_ref=line_in.at[d],
            send_sem=z_send.at[d],
            recv_sem=z_recv.at[d],
            device_id=peer,
            device_id_type=MESH,
        )
        for d, peer in enumerate(z_peers)
    ]
    far_first = sorted(range(nz - 1), key=lambda d: abs(d + 1 - nz // 2))

    for i in range(parts - 1):
        far_low[i].wait_recv()
        far_high[i].wait_recv()
        for start in chunks[i]:
            sums = far_turn(start, pieces[i], sums)
        done = begins[i] + pieces[i]
        if done in (quarter, BAND):
            send_rims(done)
        far_gram(i)
    early_at, late_at = pl.ds(0, early), pl.ds(early, slots)
    last = parts - 1
    far_low[last].wait_recv()
    far_high[last].wait_recv()
    far_gram(last)
    pack(FAR)
    late_hops = plane_sends(late_at, 3 * (nq - 1))
    for start in chunks[last]:
        sums = far_turn(start, pieces[last], sums)
    sq_own[...] = jnp.sum(sums, axis=0, keepdims=True)
    sq_hops = [
        send(
            sq_own,
            sq_plane_in.at[d],
            p_send.at[4 * (nq - 1) + d],
            p_recv.at[4 * (nq - 1) + d],
            peer,
        )
        for d, peer in enumerate(q_peers)
    ]
    for hop in early_hops:
        hop.wait_recv()
    plane_sum(early_at)
    for d in far_first:
        pl.when(slot_of[d + 1] < early)(line_copies[d].start)
    for hop in sq_hops:
        hop.wait_recv()
    value = sq_own[...]
    for d in range(nq - 1):
        value = value + sq_plane_in[d]
    sq_line[...] = value
    sq_line_hops = [
        send(sq_line, sq_line_in.at[d], z_send.at[nz - 1 + d], z_recv.at[nz - 1 + d], peer)
        for d, peer in enumerate(z_peers)
    ]
    for hop in late_hops:
        hop.wait_recv()
    plane_sum(late_at)
    for d in far_first:
        pl.when(slot_of[d + 1] >= early)(line_copies[d].start)

    def store_product(b, value):
        product[pl.ds(b * size, size), :] = value

    for hop in rims:
        hop.wait_recv()
    apply(rimmed, store_product)

    for hop in sq_line_hops:
        hop.wait_recv()
    norm = sq_line[...]
    for d in range(nz - 1):
        norm = norm + sq_line_in[d]
    scale_out[...] = lax.rsqrt(norm / vertices)
    for copy in line_copies:
        copy.wait_recv()
    value = line[slot_of[0]]
    for d in range(nz - 1):
        value = value + line_in[d]
    gram_out[...] = value / vertices
    for copy in started + line_copies:
        copy.wait_send()


def finish(
    turned, product, scale, gram, basis_out, image_out, stiff_out, mass_out, basis, image, sem
):
    rows = turned.shape[0]
    pieces = 4
    step = rows // pieces
    copies = []
    stiff_out[...] = gram[0]
    mass_out[...] = gram[1]
    for i in range(pieces):
        at = pl.ds(i * step, step)
        for j, (source, held, target) in enumerate(
            ((turned, basis, basis_out), (product, image, image_out))
        ):
            held[at, :] = (source[at, :] * scale[...]).astype(BF16)
            copy = pltpu.make_async_copy(held.at[at], target.at[at], sem.at[2 * i + j])
            copy.start()
            copies.append(copy)
    for copy in copies:
        copy.wait()


def in_hbm(value):
    return pltpu.with_memory_space_constraint(value, pltpu.HBM)


def body(basis_rows, stiff_blocks, block_neighbors, vertex_mass, rotation):
    nz, nx, _ = (lax.axis_size(a) for a in ROWS)
    ny = lax.axis_size("cols")
    rows, width = basis_rows.shape
    count, _, size, _ = stiff_blocks.shape
    pieces = (2, 2, 2, 2, 1, 1)
    parts = len(pieces)
    nq = 2 * nx
    sizes = (nz, nx, ny, count, size, width, pieces)
    reach = (count + 2 * BAND, size, width)
    vmem = pl.BlockSpec(memory_space=pltpu.VMEM)
    hbm = pl.BlockSpec(memory_space=pltpu.HBM)
    dma = pltpu.SemaphoreType.DMA
    turned, product, scale, gram = pl.pallas_call(
        functools.partial(kernel, sizes),
        out_shape=(
            jax.ShapeDtypeStruct((rows, width), F32),
            jax.ShapeDtypeStruct((rows, width), F32),
            jax.ShapeDtypeStruct((1, width), F32),
            jax.ShapeDtypeStruct((2, 4, width), F32),
        ),
        in_specs=[hbm] * 5,
        out_specs=(vmem, vmem, vmem, vmem),
        scratch_shapes=[
            pltpu.VMEM(reach, BF16),
            pltpu.VMEM((3, count, size, width), BF16),
            pltpu.VMEM(reach, BF16),
            pltpu.SMEM((3, count), jnp.int32),
            pltpu.VMEM((count, size), F32),
            pltpu.VMEM((rows, width), F32),
            pltpu.VMEM((rows, 2 * width), BF16),
            pltpu.VMEM(stiff_blocks.shape, BF16),
            pltpu.VMEM(((ny + 1) * width, width), BF16),
            pltpu.VMEM((ny, 2, width, width), F32),
            pltpu.VMEM((nq, nz, 2, 4, width), F32),
            pltpu.VMEM((nq - 1, nz, 2, 4, width), F32),
            pltpu.VMEM((nz, 2, 4, width), F32),
            pltpu.VMEM((nz - 1, 2, 4, width), F32),
            pltpu.VMEM((1, width), F32),
            pltpu.VMEM((nq - 1, 1, width), F32),
            pltpu.VMEM((1, width), F32),
            pltpu.VMEM((nz - 1, 1, width), F32),
            pltpu.SemaphoreType.REGULAR((3,)),
            dma((5 + ny,)),
            dma((4 + 2 * parts,)),
            dma((4 + 2 * parts,)),
            dma((6,)),
            dma((6,)),
            dma((5 * (nq - 1),)),
            dma((5 * (nq - 1),)),
            dma((2 * (nz - 1),)),
            dma((2 * (nz - 1),)),
        ],
        compiler_params=pltpu.CompilerParams(
            collective_id=0, has_side_effects=True, vmem_limit_bytes=VMEM_LIMIT
        ),
    )(
        in_hbm(block_neighbors.T),
        in_hbm(basis_rows.reshape(count, size, width)),
        in_hbm(stiff_blocks),
        in_hbm(vertex_mass.reshape(count, size)),
        in_hbm(rotation),
    )
    return pl.pallas_call(
        finish,
        out_shape=(
            jax.ShapeDtypeStruct((rows, width), BF16),
            jax.ShapeDtypeStruct((rows, width), BF16),
            jax.ShapeDtypeStruct((4, width), F32),
            jax.ShapeDtypeStruct((4, width), F32),
        ),
        in_specs=[vmem] * 4,
        out_specs=(hbm, hbm, vmem, vmem),
        scratch_shapes=[
            pltpu.VMEM((rows, width), BF16),
            pltpu.VMEM((rows, width), BF16),
            dma((8,)),
        ],
        compiler_params=pltpu.CompilerParams(vmem_limit_bytes=FINISH_LIMIT),
    )(turned, product, scale, gram)


def solution(mesh):
    split = Mesh(
        mesh.devices.reshape(16, 4, 2, mesh.shape["cols"]), ("rows_0", "rows_1", "rows_2", "cols")
    )
    in_specs = (P(ROWS, "cols"), P(ROWS, None, None, None), P(ROWS, None), P(ROWS), P())
    out_specs = (P(ROWS, "cols"), P(ROWS, "cols"), P(ROWS, "cols"), P(ROWS, "cols"))
    return jax.shard_map(body, mesh=split, in_specs=in_specs, out_specs=out_specs, check_vma=False)
```

```python
import functools

import jax
import jax.numpy as jnp
from jax import lax
from jax.experimental import pallas as pl
from jax.experimental.pallas import tpu as pltpu
from jax.sharding import Mesh
from jax.sharding import PartitionSpec as P

BAND = 8
ROWS = ("rows_0", "rows_1", "rows_2")
MESH = pl.DeviceIdType.MESH
F32 = jnp.float32
BF16 = jnp.bfloat16
LEFT, OWN, RIGHT, FAR = 0, 1, 2, 3
VMEM_LIMIT = 24 * 1024 * 1024
FINISH_LIMIT = 16 * 1024 * 1024


def transposed_dot(left, right):
    return lax.dot_general(left, right, (((0,), (0,)), ((), ())), preferred_element_type=F32)


def kernel(
    sizes,
    nb_hbm,
    basis_ref,
    blocks_ref,
    mass_hbm,
    rot_ref,
    turned,
    product,
    scale_out,
    gram_out,
    padded,
    others,
    rimmed,
    nb_ref,
    mass_ref,
    mass_col,
    weights,
    blocks,
    turn,
    gram,
    plane,
    plane_in,
    line,
    line_in,
    sq_own,
    sq_plane_in,
    sq_line,
    sq_line_in,
    relay,
    load_sem,
    y_send,
    y_recv,
    halo_send,
    halo_recv,
    p_send,
    p_recv,
    z_send,
    z_recv,
):
    nz, nx, ny, count, size, width, pieces = sizes
    z, x, k = (lax.axis_index(a) for a in ROWS)
    y = lax.axis_index("cols")
    half = count // 2
    parts = len(pieces)
    begins = [sum(pieces[:i]) for i in range(parts)]
    total = nz * nx * 2
    nq = 2 * nx
    q = 2 * x + k
    place = z * nq + q
    vertices = total * count * size
    slots = nz // ny
    early = nz - slots

    def row_device(index):
        index = lax.rem(index + total, total)
        return {
            "rows_0": lax.div(index, nq),
            "rows_1": lax.rem(lax.div(index, 2), nx),
            "rows_2": lax.rem(index, 2),
        }

    def along(axis, mine, length, step):
        return {axis: lax.rem(mine + length + step, length)}

    up, down = row_device(place + 1), row_device(place - 1)
    y_right, y_left = along("cols", y, ny, 1), along("cols", y, ny, -1)
    partner = {"rows_2": 1 - k}
    x_near = [along("rows_1", x, nx, d) for d in (1, -1)]
    z_near = [along("rows_0", z, nz, d) for d in (1, -1)]
    places = [lax.rem(q + d, nq) for d in range(1, nq)]
    q_peers = [{"rows_1": lax.div(p, 2), "rows_2": lax.rem(p, 2)} for p in places]
    z_peers = [along("rows_0", z, nz, d) for d in range(1, nz)]
    col_of = [lax.rem(y + ny - 1 + i, ny) for i in range(ny)]

    load_basis = pltpu.make_async_copy(basis_ref, padded.at[pl.ds(BAND, count)], load_sem.at[0])
    load_basis.start()
    load_mass = pltpu.make_async_copy(mass_hbm, mass_ref, load_sem.at[3 + ny])
    load_mass.start()
    load_nb = pltpu.make_async_copy(nb_hbm, nb_ref, load_sem.at[4 + ny])
    load_nb.start()

    peers = [y_right, y_left, partner, *x_near, *z_near]
    barrier = pltpu.get_barrier_semaphore()
    for peer in peers:
        pl.semaphore_signal(barrier, inc=1, device_id=peer, device_id_type=MESH)
    load_blocks = pltpu.make_async_copy(blocks_ref, blocks, load_sem.at[1])
    load_blocks.start()
    load_turn = []
    for i in range(ny + 1):
        load = pltpu.make_async_copy(
            rot_ref.at[
                pl.ds(pl.multiple_of(col_of[i % ny] * width, width), width),
                pl.ds(pl.multiple_of(y * width, width), width),
            ],
            turn.at[pl.ds(i * width, width)],
            load_sem.at[2 + i],
        )
        load.start()
        load_turn.append(load)
    load_basis.wait()
    pl.semaphore_wait(barrier, len(peers))

    started = []

    def send(source, target, send_sem, recv_sem, device):
        copy = pltpu.make_async_remote_copy(
            src_ref=source,
            dst_ref=target,
            send_sem=send_sem,
            recv_sem=recv_sem,
            device_id=device,
            device_id_type=MESH,
        )
        copy.start()
        started.append(copy)
        return copy

    low, high = pl.ds(0, half), pl.ds(half, half)
    mine_low, mine_high = pl.ds(BAND, half), pl.ds(BAND + half, half)
    left_first = send(
        padded.at[mine_low], others.at[0, low], y_send.at[0], y_recv.at[0], y_right
    )
    right_first = send(
        padded.at[mine_high], others.at[1, high], y_send.at[1], y_recv.at[1], y_left
    )
    left_second = send(
        padded.at[mine_high], others.at[0, high], y_send.at[2], y_recv.at[2], y_right
    )
    right_second = send(
        padded.at[mine_low], others.at[1, low], y_send.at[3], y_recv.at[3], y_left
    )

    relays = [
        [*z_near, *x_near, partner],
        [z_peers[1], z_peers[nz - 3], *x_near, partner],
        [z_peers[3], z_peers[nz - 5]],
    ]

    def tell(i):
        for peer in relays[i]:
            pl.semaphore_signal(relay.at[i], inc=1, device_id=peer, device_id_type=MESH)

    def hear(i):
        pl.semaphore_wait(relay.at[i], len(relays[i]))

    def weigh(b):
        at = pl.ds(b * size, size)
        column = jnp.broadcast_to(mass_ref[b : b + 1, :], (size, size)).T
        mass_col[at, :] = column
        weights[at, width:] = (column * padded[BAND + b].astype(F32)).astype(BF16)

    tell(0)
    load_mass.wait()
    for b in range(half):
        weigh(b)
    hear(0)
    tell(1)
    for b in range(half, count):
        weigh(b)
    hear(1)
    first_rows, last_rows = pl.ds(BAND, BAND), pl.ds(count, BAND)
    before, after = pl.ds(0, BAND), pl.ds(BAND + count, BAND)
    halo_low = send(
        padded.at[last_rows], padded.at[before], halo_send.at[0], halo_recv.at[0], up
    )
    halo_high = send(
        padded.at[first_rows], padded.at[after], halo_send.at[1], halo_recv.at[1], down
    )
    tell(2)

    def apply(source, store):
        for b in range(count):
            matrix = jnp.concatenate([blocks[b, n] for n in range(3)], axis=1)
            tiles = []
            for n in range(3):
                local = nb_ref[n, b] - place * count + BAND
                local = jnp.minimum(jnp.maximum(local, 0), count + 2 * BAND - 1)
                tiles.append(source[local])
            value = jnp.dot(
                matrix, jnp.concatenate(tiles, axis=0), preferred_element_type=F32
            )
            store(b, value)

    def store_image(b, value):
        weights[pl.ds(b * size, size), :width] = value.astype(BF16)

    load_blocks.wait()
    load_nb.wait()
    halo_low.wait_recv()
    halo_high.wait_recv()
    apply(padded, store_image)
    hear(2)

    def add_gram(which, source, start, length, fresh):
        part = transposed_dot(source, weights[pl.ds(start * size, length * size), :])
        for j in range(2):
            value = part[:, j * width : (j + 1) * width]
            gram[which, j] = value if fresh else gram[which, j] + value

    def some(ref, start, length):
        return ref[pl.ds(start, length)].reshape(length * size, width)

    def pack(which):
        for t in range(width // 8):
            for j in range(2):
                value = gram[which, j, pl.ds(8 * t, 8), :]
                at = slots * which + t // nx
                plane[2 * (t % nx), at, j] = value[:4]
                plane[2 * (t % nx) + 1, at, j] = value[4:]

    def plane_sends(at, offset):
        return [
            send(
                plane.at[places[d], at],
                plane_in.at[d, at],
                p_send.at[offset + d],
                p_recv.at[offset + d],
                peer,
            )
            for d, peer in enumerate(q_peers)
        ]

    def plane_sum(at):
        value = plane[q, at]
        for d in range(nq - 1):
            value = value + plane_in[d, at]
        line[at] = value

    at_piece = [pl.ds(slots * i, slots) for i in range(ny)]
    left_first.wait_recv()
    right_first.wait_recv()
    chunks = []
    far_low, far_high = [], []
    for i in range(parts):
        starts = (begins[i], count - begins[i] - pieces[i])
        chunks.append(starts)
        at = pl.ds(starts[0], pieces[i])
        j = 4 + i
        far_low.append(
            send(others.at[0, at], others.at[2, at], y_send.at[j], y_recv.at[j], y_right)
        )
        at = pl.ds(starts[1], pieces[i])
        j = 4 + parts + i
        far_high.append(
            send(others.at[1, at], others.at[2, at], y_send.at[j], y_recv.at[j], y_left)
        )
    left, right, far = (others.at[i] for i in range(3))
    step = count // 4
    for i in range(4):
        add_gram(OWN, some(padded, BAND + i * step, step), i * step, step, i == 0)

    pack(OWN)
    early_hops = plane_sends(at_piece[OWN], 0)
    for i in range(2):
        add_gram(LEFT, some(left, i * step, step), i * step, step, i == 0)
    for i in range(2, 4):
        add_gram(RIGHT, some(right, i * step, step), i * step, step, i == 2)
    for load in load_turn:
        load.wait()
    for i in range(count // 2):
        own = some(padded, BAND + 2 * i, 2)
        if 2 * i < half:
            pair, at = [some(left, 2 * i, 2), own], pl.ds(0, 2 * width)
        else:
            pair, at = [own, some(right, 2 * i, 2)], pl.ds(width, 2 * width)
        turned[pl.ds(2 * i * size, 2 * size), :] = jnp.dot(
            jnp.concatenate(pair, axis=1), turn[at, :], preferred_element_type=F32
        )
    left_second.wait_recv()
    right_second.wait_recv()
    for i in range(2, 4):
        add_gram(LEFT, some(left, i * step, step), i * step, step, False)
    for i in range(2):
        add_gram(RIGHT, some(right, i * step, step), i * step, step, False)

    pack(LEFT)
    early_hops += plane_sends(at_piece[LEFT], nq - 1)
    pack(RIGHT)
    early_hops += plane_sends(at_piece[RIGHT], 2 * (nq - 1))

    sums = jnp.zeros((8, width), F32)

    def far_turn(start, piece, sums):
        at = pl.ds(start * size, piece * size)
        if start < half:
            pair, place_of = [some(right, start, piece), some(far, start, piece)], 2
        else:
            pair, place_of = [some(far, start, piece), some(left, start, piece)], 3
        value = turned[at, :] + jnp.dot(
            jnp.concatenate(pair, axis=1),
            turn[pl.ds(place_of * width, 2 * width), :],
            preferred_element_type=F32,
        )
        turned[at, :] = value
        rimmed[pl.ds(BAND + start, piece)] = value.astype(BF16).reshape(piece, size, width)
        squares = mass_col[at, :] * value * value
        return sums + jnp.sum(squares.reshape(piece * size // 8, 8, width), axis=0)

    rims = []
    quarter = BAND // 2
    def send_rims(done):
        j = 2 + 2 * (done // quarter - 1)
        rims.append(
            send(
                rimmed.at[pl.ds(BAND + done - quarter, quarter)],
                rimmed.at[pl.ds(BAND + count + done - quarter, quarter)],
                halo_send.at[j],
                halo_recv.at[j],
                down,
            )
        )
        rims.append(
            send(
                rimmed.at[pl.ds(BAND + count - done, quarter)],
                rimmed.at[pl.ds(BAND - done, quarter)],
                halo_send.at[j + 1],
                halo_recv.at[j + 1],
                up,
            )
        )

    def far_gram(i):
        for j, start in enumerate(chunks[i]):
            source = some(far, start, pieces[i])
            add_gram(FAR, source, start, pieces[i], i == 0 and j == 0)

    slot_of = [lax.rem(z + d + slots + nz - slots * y, nz) for d in range(nz)]
    line_copies = [
        pltpu.make_async_remote_copy(
            src_ref=line.at[slot_of[d + 1]],
            dst_ref=line_in.at[d],
            send_sem=z_send.at[d],
            recv_sem=z_recv.at[d],
            device_id=peer,
            device_id_type=MESH,
        )
        for d, peer in enumerate(z_peers)
    ]
    far_first = sorted(range(nz - 1), key=lambda d: abs(d + 1 - nz // 2))

    for i in range(parts - 1):
        far_low[i].wait_recv()
        far_high[i].wait_recv()
        for start in chunks[i]:
            sums = far_turn(start, pieces[i], sums)
        if begins[i] + pieces[i] == quarter:
            send_rims(quarter)
        far_gram(i)
    early_at, late_at = pl.ds(0, early), pl.ds(early, slots)
    last = parts - 1
    far_low[last].wait_recv()
    far_high[last].wait_recv()
    far_gram(last)
    pack(FAR)
    late_hops = plane_sends(late_at, 3 * (nq - 1))
    for start in chunks[last]:
        sums = far_turn(start, pieces[last], sums)
    sq_own[...] = jnp.sum(sums, axis=0, keepdims=True)
    sq_hops = [
        send(
            sq_own,
            sq_plane_in.at[d],
            p_send.at[4 * (nq - 1) + d],
            p_recv.at[4 * (nq - 1) + d],
            peer,
        )
        for d, peer in enumerate(q_peers)
    ]
    send_rims(BAND)
    for hop in early_hops:
        hop.wait_recv()
    plane_sum(early_at)
    for d in far_first:
        pl.when(slot_of[d + 1] < early)(line_copies[d].start)
    for hop in sq_hops:
        hop.wait_recv()
    value = sq_own[...]
    for d in range(nq - 1):
        value = value + sq_plane_in[d]
    sq_line[...] = value
    sq_line_hops = [
        send(sq_line, sq_line_in.at[d], z_send.at[nz - 1 + d], z_recv.at[nz - 1 + d], peer)
        for d, peer in enumerate(z_peers)
    ]
    for hop in late_hops:
        hop.wait_recv()
    plane_sum(late_at)
    for d in far_first:
        pl.when(slot_of[d + 1] >= early)(line_copies[d].start)

    def store_product(b, value):
        product[pl.ds(b * size, size), :] = value

    for hop in rims:
        hop.wait_recv()
    apply(rimmed, store_product)

    for hop in sq_line_hops:
        hop.wait_recv()
    norm = sq_line[...]
    for d in range(nz - 1):
        norm = norm + sq_line_in[d]
    scale_out[...] = lax.rsqrt(norm / vertices)
    for copy in line_copies:
        copy.wait_recv()
    value = line[slot_of[0]]
    for d in range(nz - 1):
        value = value + line_in[d]
    gram_out[...] = value / vertices
    for copy in started + line_copies:
        copy.wait_send()


def finish(
    turned, product, scale, gram, basis_out, image_out, stiff_out, mass_out, basis, image, sem
):
    rows = turned.shape[0]
    pieces = 4
    step = rows // pieces
    copies = []
    stiff_out[...] = gram[0]
    mass_out[...] = gram[1]
    for i in range(pieces):
        at = pl.ds(i * step, step)
        for j, (source, held, target) in enumerate(
            ((turned, basis, basis_out), (product, image, image_out))
        ):
            held[at, :] = (source[at, :] * scale[...]).astype(BF16)
            copy = pltpu.make_async_copy(held.at[at], target.at[at], sem.at[2 * i + j])
            copy.start()
            copies.append(copy)
    for copy in copies:
        copy.wait()


def in_hbm(value):
    return pltpu.with_memory_space_constraint(value, pltpu.HBM)


def body(basis_rows, stiff_blocks, block_neighbors, vertex_mass, rotation):
    nz, nx, _ = (lax.axis_size(a) for a in ROWS)
    ny = lax.axis_size("cols")
    rows, width = basis_rows.shape
    count, _, size, _ = stiff_blocks.shape
    pieces = (2, 2, 2, 2, 1, 1)
    parts = len(pieces)
    nq = 2 * nx
    sizes = (nz, nx, ny, count, size, width, pieces)
    reach = (count + 2 * BAND, size, width)
    vmem = pl.BlockSpec(memory_space=pltpu.VMEM)
    hbm = pl.BlockSpec(memory_space=pltpu.HBM)
    dma = pltpu.SemaphoreType.DMA
    turned, product, scale, gram = pl.pallas_call(
        functools.partial(kernel, sizes),
        out_shape=(
            jax.ShapeDtypeStruct((rows, width), F32),
            jax.ShapeDtypeStruct((rows, width), F32),
            jax.ShapeDtypeStruct((1, width), F32),
            jax.ShapeDtypeStruct((2, 4, width), F32),
        ),
        in_specs=[hbm] * 5,
        out_specs=(vmem, vmem, vmem, vmem),
        scratch_shapes=[
            pltpu.VMEM(reach, BF16),
            pltpu.VMEM((3, count, size, width), BF16),
            pltpu.VMEM(reach, BF16),
            pltpu.SMEM((3, count), jnp.int32),
            pltpu.VMEM((count, size), F32),
            pltpu.VMEM((rows, width), F32),
            pltpu.VMEM((rows, 2 * width), BF16),
            pltpu.VMEM(stiff_blocks.shape, BF16),
            pltpu.VMEM(((ny + 1) * width, width), BF16),
            pltpu.VMEM((ny, 2, width, width), F32),
            pltpu.VMEM((nq, nz, 2, 4, width), F32),
            pltpu.VMEM((nq - 1, nz, 2, 4, width), F32),
            pltpu.VMEM((nz, 2, 4, width), F32),
            pltpu.VMEM((nz - 1, 2, 4, width), F32),
            pltpu.VMEM((1, width), F32),
            pltpu.VMEM((nq - 1, 1, width), F32),
            pltpu.VMEM((1, width), F32),
            pltpu.VMEM((nz - 1, 1, width), F32),
            pltpu.SemaphoreType.REGULAR((3,)),
            dma((5 + ny,)),
            dma((4 + 2 * parts,)),
            dma((4 + 2 * parts,)),
            dma((6,)),
            dma((6,)),
            dma((5 * (nq - 1),)),
            dma((5 * (nq - 1),)),
            dma((2 * (nz - 1),)),
            dma((2 * (nz - 1),)),
        ],
        compiler_params=pltpu.CompilerParams(
            collective_id=0, has_side_effects=True, vmem_limit_bytes=VMEM_LIMIT
        ),
    )(
        in_hbm(block_neighbors.T),
        in_hbm(basis_rows.reshape(count, size, width)),
        in_hbm(stiff_blocks),
        in_hbm(vertex_mass.reshape(count, size)),
        in_hbm(rotation),
    )
    return pl.pallas_call(
        finish,
        out_shape=(
            jax.ShapeDtypeStruct((rows, width), BF16),
            jax.ShapeDtypeStruct((rows, width), BF16),
            jax.ShapeDtypeStruct((4, width), F32),
            jax.ShapeDtypeStruct((4, width), F32),
        ),
        in_specs=[vmem] * 4,
        out_specs=(hbm, hbm, vmem, vmem),
        scratch_shapes=[
            pltpu.VMEM((rows, width), BF16),
            pltpu.VMEM((rows, width), BF16),
            dma((8,)),
        ],
        compiler_params=pltpu.CompilerParams(vmem_limit_bytes=FINISH_LIMIT),
    )(turned, product, scale, gram)


def solution(mesh):
    split = Mesh(
        mesh.devices.reshape(16, 4, 2, mesh.shape["cols"]), ("rows_0", "rows_1", "rows_2", "cols")
    )
    in_specs = (P(ROWS, "cols"), P(ROWS, None, None, None), P(ROWS, None), P(ROWS), P())
    out_specs = (P(ROWS, "cols"), P(ROWS, "cols"), P(ROWS, "cols"), P(ROWS, "cols"))
    return jax.shard_map(body, mesh=split, in_specs=in_specs, out_specs=out_specs, check_vma=False)
```

```python
import functools

import jax
import jax.numpy as jnp
from jax import lax
from jax.experimental import pallas as pl
from jax.experimental.pallas import tpu as pltpu
from jax.sharding import Mesh
from jax.sharding import PartitionSpec as P

BAND = 8
ROWS = ("rows_0", "rows_1", "rows_2")
MESH = pl.DeviceIdType.MESH
F32 = jnp.float32
BF16 = jnp.bfloat16
LEFT, OWN, RIGHT, FAR = 0, 1, 2, 3
VMEM_LIMIT = 24 * 1024 * 1024
FINISH_LIMIT = 16 * 1024 * 1024


def transposed_dot(left, right):
    return lax.dot_general(left, right, (((0,), (0,)), ((), ())), preferred_element_type=F32)


def kernel(
    sizes,
    nb_hbm,
    basis_ref,
    blocks_ref,
    mass_hbm,
    rot_ref,
    turned,
    product,
    scale_out,
    gram_out,
    padded,
    others,
    rimmed,
    nb_ref,
    mass_ref,
    mass_col,
    weights,
    blocks,
    turn,
    gram,
    plane,
    plane_in,
    line,
    line_in,
    sq_own,
    sq_plane_in,
    sq_line,
    sq_line_in,
    relay,
    load_sem,
    y_send,
    y_recv,
    halo_send,
    halo_recv,
    p_send,
    p_recv,
    z_send,
    z_recv,
):
    nz, nx, ny, count, size, width, pieces = sizes
    z, x, k = (lax.axis_index(a) for a in ROWS)
    y = lax.axis_index("cols")
    half = count // 2
    parts = len(pieces)
    begins = [sum(pieces[:i]) for i in range(parts)]
    total = nz * nx * 2
    nq = 2 * nx
    q = 2 * x + k
    place = z * nq + q
    vertices = total * count * size
    slots = nz // ny
    early = nz - slots

    def row_device(index):
        index = lax.rem(index + total, total)
        return {
            "rows_0": lax.div(index, nq),
            "rows_1": lax.rem(lax.div(index, 2), nx),
            "rows_2": lax.rem(index, 2),
        }

    def along(axis, mine, length, step):
        return {axis: lax.rem(mine + length + step, length)}

    up, down = row_device(place + 1), row_device(place - 1)
    y_right, y_left = along("cols", y, ny, 1), along("cols", y, ny, -1)
    partner = {"rows_2": 1 - k}
    x_near = [along("rows_1", x, nx, d) for d in (1, -1)]
    z_near = [along("rows_0", z, nz, d) for d in (1, -1)]
    places = [lax.rem(q + d, nq) for d in range(1, nq)]
    q_peers = [{"rows_1": lax.div(p, 2), "rows_2": lax.rem(p, 2)} for p in places]
    z_peers = [along("rows_0", z, nz, d) for d in range(1, nz)]
    col_of = [lax.rem(y + ny - 1 + i, ny) for i in range(ny)]

    load_basis = pltpu.make_async_copy(basis_ref, padded.at[pl.ds(BAND, count)], load_sem.at[0])
    load_basis.start()
    load_mass = pltpu.make_async_copy(mass_hbm, mass_ref, load_sem.at[3 + ny])
    load_mass.start()
    load_nb = pltpu.make_async_copy(nb_hbm, nb_ref, load_sem.at[4 + ny])
    load_nb.start()

    peers = [y_right, y_left, partner, *x_near, *z_near]
    barrier = pltpu.get_barrier_semaphore()
    for peer in peers:
        pl.semaphore_signal(barrier, inc=1, device_id=peer, device_id_type=MESH)
    load_blocks = pltpu.make_async_copy(blocks_ref, blocks, load_sem.at[1])
    load_blocks.start()
    load_turn = []
    for i in range(ny + 1):
        load = pltpu.make_async_copy(
            rot_ref.at[
                pl.ds(pl.multiple_of(col_of[i % ny] * width, width), width),
                pl.ds(pl.multiple_of(y * width, width), width),
            ],
            turn.at[pl.ds(i * width, width)],
            load_sem.at[2 + i],
        )
        load.start()
        load_turn.append(load)
    load_basis.wait()
    pl.semaphore_wait(barrier, len(peers))

    started = []

    def send(source, target, send_sem, recv_sem, device):
        copy = pltpu.make_async_remote_copy(
            src_ref=source,
            dst_ref=target,
            send_sem=send_sem,
            recv_sem=recv_sem,
            device_id=device,
            device_id_type=MESH,
        )
        copy.start()
        started.append(copy)
        return copy

    low, high = pl.ds(0, half), pl.ds(half, half)
    mine_low, mine_high = pl.ds(BAND, half), pl.ds(BAND + half, half)
    left_first = send(
        padded.at[mine_low], others.at[0, low], y_send.at[0], y_recv.at[0], y_right
    )
    right_first = send(
        padded.at[mine_high], others.at[1, high], y_send.at[1], y_recv.at[1], y_left
    )
    left_second = send(
        padded.at[mine_high], others.at[0, high], y_send.at[2], y_recv.at[2], y_right
    )
    right_second = send(
        padded.at[mine_low], others.at[1, low], y_send.at[3], y_recv.at[3], y_left
    )

    relays = [
        [*z_near, *x_near, partner],
        [z_peers[1], z_peers[nz - 3], *x_near, partner],
        [z_peers[3], z_peers[nz - 5]],
    ]

    def tell(i):
        for peer in relays[i]:
            pl.semaphore_signal(relay.at[i], inc=1, device_id=peer, device_id_type=MESH)

    def hear(i):
        pl.semaphore_wait(relay.at[i], len(relays[i]))

    def weigh(b):
        at = pl.ds(b * size, size)
        column = jnp.broadcast_to(mass_ref[b : b + 1, :], (size, size)).T
        mass_col[at, :] = column
        weights[at, width:] = (column * padded[BAND + b].astype(F32)).astype(BF16)

    tell(0)
    load_mass.wait()
    for b in range(half):
        weigh(b)
    hear(0)
    tell(1)
    for b in range(half, count):
        weigh(b)
    hear(1)
    first_rows, last_rows = pl.ds(BAND, BAND), pl.ds(count, BAND)
    before, after = pl.ds(0, BAND), pl.ds(BAND + count, BAND)
    halo_low = send(
        padded.at[last_rows], padded.at[before], halo_send.at[0], halo_recv.at[0], up
    )
    halo_high = send(
        padded.at[first_rows], padded.at[after], halo_send.at[1], halo_recv.at[1], down
    )
    tell(2)

    def apply(source, store):
        for b in range(count):
            matrix = jnp.concatenate([blocks[b, n] for n in range(3)], axis=1)
            tiles = []
            for n in range(3):
                local = nb_ref[n, b] - place * count + BAND
                local = jnp.minimum(jnp.maximum(local, 0), count + 2 * BAND - 1)
                tiles.append(source[local])
            value = jnp.dot(
                matrix, jnp.concatenate(tiles, axis=0), preferred_element_type=F32
            )
            store(b, value)

    def store_image(b, value):
        weights[pl.ds(b * size, size), :width] = value.astype(BF16)

    load_blocks.wait()
    load_nb.wait()
    halo_low.wait_recv()
    halo_high.wait_recv()
    apply(padded, store_image)
    hear(2)

    def add_gram(which, source, start, length, fresh):
        part = transposed_dot(source, weights[pl.ds(start * size, length * size), :])
        for j in range(2):
            value = part[:, j * width : (j + 1) * width]
            gram[which, j] = value if fresh else gram[which, j] + value

    def some(ref, start, length):
        return ref[pl.ds(start, length)].reshape(length * size, width)

    def pack(which):
        for t in range(width // 8):
            stiff, mass = (gram[which, j, pl.ds(8 * t, 8), :] for j in range(2))
            at = slots * which + t // nx
            for c in range(2):
                rows = slice(4 * c, 4 * c + 4)
                both = jnp.concatenate([stiff[rows], mass[rows]], axis=0)
                plane[2 * (t % nx) + c, at] = both.astype(BF16)

    def plane_sends(at, offset):
        return [
            send(
                plane.at[places[d], at],
                plane_in.at[d, at],
                p_send.at[offset + d],
                p_recv.at[offset + d],
                peer,
            )
            for d, peer in enumerate(q_peers)
        ]

    def plane_sum(at):
        value = plane[q, at].astype(F32)
        for d in range(nq - 1):
            value = value + plane_in[d, at].astype(F32)
        line[at] = value

    at_piece = [pl.ds(slots * i, slots) for i in range(ny)]
    left_first.wait_recv()
    right_first.wait_recv()
    chunks = []
    far_low, far_high = [], []
    for i in range(parts):
        starts = (begins[i], count - begins[i] - pieces[i])
        chunks.append(starts)
        at = pl.ds(starts[0], pieces[i])
        j = 4 + i
        far_low.append(
            send(others.at[0, at], others.at[2, at], y_send.at[j], y_recv.at[j], y_right)
        )
        at = pl.ds(starts[1], pieces[i])
        j = 4 + parts + i
        far_high.append(
            send(others.at[1, at], others.at[2, at], y_send.at[j], y_recv.at[j], y_left)
        )
    left, right, far = (others.at[i] for i in range(3))
    step = count // 4
    for i in range(4):
        add_gram(OWN, some(padded, BAND + i * step, step), i * step, step, i == 0)

    pack(OWN)
    early_hops = plane_sends(at_piece[OWN], 0)
    for i in range(2):
        add_gram(LEFT, some(left, i * step, step), i * step, step, i == 0)
    for i in range(2, 4):
        add_gram(RIGHT, some(right, i * step, step), i * step, step, i == 2)
    for load in load_turn:
        load.wait()
    for i in range(count // 2):
        own = some(padded, BAND + 2 * i, 2)
        if 2 * i < half:
            pair, at = [some(left, 2 * i, 2), own], pl.ds(0, 2 * width)
        else:
            pair, at = [own, some(right, 2 * i, 2)], pl.ds(width, 2 * width)
        turned[pl.ds(2 * i * size, 2 * size), :] = jnp.dot(
            jnp.concatenate(pair, axis=1), turn[at, :], preferred_element_type=F32
        )
    left_second.wait_recv()
    right_second.wait_recv()
    for i in range(2, 4):
        add_gram(LEFT, some(left, i * step, step), i * step, step, False)
    for i in range(2):
        add_gram(RIGHT, some(right, i * step, step), i * step, step, False)

    pack(LEFT)
    early_hops += plane_sends(at_piece[LEFT], nq - 1)
    pack(RIGHT)
    early_hops += plane_sends(at_piece[RIGHT], 2 * (nq - 1))

    sums = jnp.zeros((8, width), F32)

    def far_turn(start, piece, sums):
        at = pl.ds(start * size, piece * size)
        if start < half:
            pair, place_of = [some(right, start, piece), some(far, start, piece)], 2
        else:
            pair, place_of = [some(far, start, piece), some(left, start, piece)], 3
        value = turned[at, :] + jnp.dot(
            jnp.concatenate(pair, axis=1),
            turn[pl.ds(place_of * width, 2 * width), :],
            preferred_element_type=F32,
        )
        turned[at, :] = value
        rimmed[pl.ds(BAND + start, piece)] = value.astype(BF16).reshape(piece, size, width)
        squares = mass_col[at, :] * value * value
        return sums + jnp.sum(squares.reshape(piece * size // 8, 8, width), axis=0)

    rims = []
    quarter = BAND // 2
    def send_rims(done):
        j = 2 + 2 * (done // quarter - 1)
        rims.append(
            send(
                rimmed.at[pl.ds(BAND + done - quarter, quarter)],
                rimmed.at[pl.ds(BAND + count + done - quarter, quarter)],
                halo_send.at[j],
                halo_recv.at[j],
                down,
            )
        )
        rims.append(
            send(
                rimmed.at[pl.ds(BAND + count - done, quarter)],
                rimmed.at[pl.ds(BAND - done, quarter)],
                halo_send.at[j + 1],
                halo_recv.at[j + 1],
                up,
            )
        )

    def far_gram(i):
        for j, start in enumerate(chunks[i]):
            source = some(far, start, pieces[i])
            add_gram(FAR, source, start, pieces[i], i == 0 and j == 0)

    slot_of = [lax.rem(z + d + slots + nz - slots * y, nz) for d in range(nz)]
    line_copies = [
        pltpu.make_async_remote_copy(
            src_ref=line.at[slot_of[d + 1]],
            dst_ref=line_in.at[d],
            send_sem=z_send.at[d],
            recv_sem=z_recv.at[d],
            device_id=peer,
            device_id_type=MESH,
        )
        for d, peer in enumerate(z_peers)
    ]
    far_first = sorted(range(nz - 1), key=lambda d: abs(d + 1 - nz // 2))

    for i in range(parts - 1):
        far_low[i].wait_recv()
        far_high[i].wait_recv()
        for start in chunks[i]:
            sums = far_turn(start, pieces[i], sums)
        done = begins[i] + pieces[i]
        if done in (quarter, BAND):
            send_rims(done)
        far_gram(i)
    early_at, late_at = pl.ds(0, early), pl.ds(early, slots)
    last = parts - 1
    far_low[last].wait_recv()
    far_high[last].wait_recv()
    far_gram(last)
    pack(FAR)
    late_hops = plane_sends(late_at, 3 * (nq - 1))
    for start in chunks[last]:
        sums = far_turn(start, pieces[last], sums)
    sq_own[...] = jnp.sum(sums, axis=0, keepdims=True)
    sq_hops = [
        send(
            sq_own,
            sq_plane_in.at[d],
            p_send.at[4 * (nq - 1) + d],
            p_recv.at[4 * (nq - 1) + d],
            peer,
        )
        for d, peer in enumerate(q_peers)
    ]
    for hop in early_hops:
        hop.wait_recv()
    plane_sum(early_at)
    for d in far_first:
        pl.when(slot_of[d + 1] < early)(line_copies[d].start)
    for hop in sq_hops:
        hop.wait_recv()
    value = sq_own[...]
    for d in range(nq - 1):
        value = value + sq_plane_in[d]
    sq_line[...] = value
    sq_line_hops = [
        send(sq_line, sq_line_in.at[d], z_send.at[nz - 1 + d], z_recv.at[nz - 1 + d], peer)
        for d, peer in enumerate(z_peers)
    ]
    for hop in late_hops:
        hop.wait_recv()
    plane_sum(late_at)
    for d in far_first:
        pl.when(slot_of[d + 1] >= early)(line_copies[d].start)

    def store_product(b, value):
        product[pl.ds(b * size, size), :] = value

    for hop in rims:
        hop.wait_recv()
    apply(rimmed, store_product)

    for hop in sq_line_hops:
        hop.wait_recv()
    norm = sq_line[...]
    for d in range(nz - 1):
        norm = norm + sq_line_in[d]
    scale_out[...] = lax.rsqrt(norm / vertices)
    for copy in line_copies:
        copy.wait_recv()
    value = line[slot_of[0]]
    for d in range(nz - 1):
        value = value + line_in[d]
    gram_out[...] = value / vertices
    for copy in started + line_copies:
        copy.wait_send()


def finish(
    turned, product, scale, gram, basis_out, image_out, stiff_out, mass_out, basis, image, sem
):
    rows = turned.shape[0]
    pieces = 4
    step = rows // pieces
    copies = []
    stiff_out[...] = gram[:4, :]
    mass_out[...] = gram[4:, :]
    for i in range(pieces):
        at = pl.ds(i * step, step)
        for j, (source, held, target) in enumerate(
            ((turned, basis, basis_out), (product, image, image_out))
        ):
            held[at, :] = (source[at, :] * scale[...]).astype(BF16)
            copy = pltpu.make_async_copy(held.at[at], target.at[at], sem.at[2 * i + j])
            copy.start()
            copies.append(copy)
    for copy in copies:
        copy.wait()


def in_hbm(value):
    return pltpu.with_memory_space_constraint(value, pltpu.HBM)


def body(basis_rows, stiff_blocks, block_neighbors, vertex_mass, rotation):
    nz, nx, _ = (lax.axis_size(a) for a in ROWS)
    ny = lax.axis_size("cols")
    rows, width = basis_rows.shape
    count, _, size, _ = stiff_blocks.shape
    pieces = (2, 2, 2, 2, 1, 1)
    parts = len(pieces)
    nq = 2 * nx
    sizes = (nz, nx, ny, count, size, width, pieces)
    reach = (count + 2 * BAND, size, width)
    vmem = pl.BlockSpec(memory_space=pltpu.VMEM)
    hbm = pl.BlockSpec(memory_space=pltpu.HBM)
    dma = pltpu.SemaphoreType.DMA
    turned, product, scale, gram = pl.pallas_call(
        functools.partial(kernel, sizes),
        out_shape=(
            jax.ShapeDtypeStruct((rows, width), F32),
            jax.ShapeDtypeStruct((rows, width), F32),
            jax.ShapeDtypeStruct((1, width), F32),
            jax.ShapeDtypeStruct((8, width), F32),
        ),
        in_specs=[hbm] * 5,
        out_specs=(vmem, vmem, vmem, vmem),
        scratch_shapes=[
            pltpu.VMEM(reach, BF16),
            pltpu.VMEM((3, count, size, width), BF16),
            pltpu.VMEM(reach, BF16),
            pltpu.SMEM((3, count), jnp.int32),
            pltpu.VMEM((count, size), F32),
            pltpu.VMEM((rows, width), F32),
            pltpu.VMEM((rows, 2 * width), BF16),
            pltpu.VMEM(stiff_blocks.shape, BF16),
            pltpu.VMEM(((ny + 1) * width, width), BF16),
            pltpu.VMEM((ny, 2, width, width), F32),
            pltpu.VMEM((nq, nz, 8, width), BF16),
            pltpu.VMEM((nq - 1, nz, 8, width), BF16),
            pltpu.VMEM((nz, 8, width), F32),
            pltpu.VMEM((nz - 1, 8, width), F32),
            pltpu.VMEM((1, width), F32),
            pltpu.VMEM((nq - 1, 1, width), F32),
            pltpu.VMEM((1, width), F32),
            pltpu.VMEM((nz - 1, 1, width), F32),
            pltpu.SemaphoreType.REGULAR((3,)),
            dma((5 + ny,)),
            dma((4 + 2 * parts,)),
            dma((4 + 2 * parts,)),
            dma((6,)),
            dma((6,)),
            dma((5 * (nq - 1),)),
            dma((5 * (nq - 1),)),
            dma((2 * (nz - 1),)),
            dma((2 * (nz - 1),)),
        ],
        compiler_params=pltpu.CompilerParams(
            collective_id=0, has_side_effects=True, vmem_limit_bytes=VMEM_LIMIT
        ),
    )(
        in_hbm(block_neighbors.T),
        in_hbm(basis_rows.reshape(count, size, width)),
        in_hbm(stiff_blocks),
        in_hbm(vertex_mass.reshape(count, size)),
        in_hbm(rotation),
    )
    return pl.pallas_call(
        finish,
        out_shape=(
            jax.ShapeDtypeStruct((rows, width), BF16),
            jax.ShapeDtypeStruct((rows, width), BF16),
            jax.ShapeDtypeStruct((4, width), F32),
            jax.ShapeDtypeStruct((4, width), F32),
        ),
        in_specs=[vmem] * 4,
        out_specs=(hbm, hbm, vmem, vmem),
        scratch_shapes=[
            pltpu.VMEM((rows, width), BF16),
            pltpu.VMEM((rows, width), BF16),
            dma((8,)),
        ],
        compiler_params=pltpu.CompilerParams(vmem_limit_bytes=FINISH_LIMIT),
    )(turned, product, scale, gram)


def solution(mesh):
    split = Mesh(
        mesh.devices.reshape(16, 4, 2, mesh.shape["cols"]), ("rows_0", "rows_1", "rows_2", "cols")
    )
    in_specs = (P(ROWS, "cols"), P(ROWS, None, None, None), P(ROWS, None), P(ROWS), P())
    out_specs = (P(ROWS, "cols"), P(ROWS, "cols"), P(ROWS, "cols"), P(ROWS, "cols"))
    return jax.shard_map(body, mesh=split, in_specs=in_specs, out_specs=out_specs, check_vma=False)
```

```python
import functools

import jax
import jax.numpy as jnp
from jax import lax
from jax.experimental import pallas as pl
from jax.experimental.pallas import tpu as pltpu
from jax.sharding import Mesh
from jax.sharding import PartitionSpec as P

BAND = 8
ROWS = ("rows_0", "rows_1", "rows_2")
MESH = pl.DeviceIdType.MESH
F32 = jnp.float32
BF16 = jnp.bfloat16
LEFT, OWN, RIGHT, FAR = 0, 1, 2, 3
VMEM_LIMIT = 24 * 1024 * 1024
FINISH_LIMIT = 16 * 1024 * 1024


def transposed_dot(left, right):
    return lax.dot_general(left, right, (((0,), (0,)), ((), ())), preferred_element_type=F32)


def kernel(
    sizes,
    nb_hbm,
    basis_ref,
    blocks_ref,
    mass_hbm,
    rot_ref,
    turned,
    product,
    scale_out,
    gram_out,
    padded,
    others,
    rimmed,
    nb_ref,
    mass_ref,
    mass_col,
    weights,
    blocks,
    turn,
    gram,
    plane,
    plane_in,
    line,
    line_in,
    sq_own,
    sq_plane_in,
    sq_line,
    sq_line_in,
    relay,
    load_sem,
    y_send,
    y_recv,
    halo_send,
    halo_recv,
    p_send,
    p_recv,
    z_send,
    z_recv,
):
    nz, nx, ny, count, size, width, pieces = sizes
    z, x, k = (lax.axis_index(a) for a in ROWS)
    y = lax.axis_index("cols")
    half = count // 2
    parts = len(pieces)
    begins = [sum(pieces[:i]) for i in range(parts)]
    total = nz * nx * 2
    nq = 2 * nx
    q = 2 * x + k
    place = z * nq + q
    vertices = total * count * size
    slots = nz // ny
    early = nz - slots

    def row_device(index):
        index = lax.rem(index + total, total)
        return {
            "rows_0": lax.div(index, nq),
            "rows_1": lax.rem(lax.div(index, 2), nx),
            "rows_2": lax.rem(index, 2),
        }

    def along(axis, mine, length, step):
        return {axis: lax.rem(mine + length + step, length)}

    up, down = row_device(place + 1), row_device(place - 1)
    y_right, y_left = along("cols", y, ny, 1), along("cols", y, ny, -1)
    partner = {"rows_2": 1 - k}
    x_near = [along("rows_1", x, nx, d) for d in (1, -1)]
    z_near = [along("rows_0", z, nz, d) for d in (1, -1)]
    places = [lax.rem(q + d, nq) for d in range(1, nq)]
    q_peers = [{"rows_1": lax.div(p, 2), "rows_2": lax.rem(p, 2)} for p in places]
    z_peers = [along("rows_0", z, nz, d) for d in range(1, nz)]
    col_of = [lax.rem(y + ny - 1 + i, ny) for i in range(ny)]

    load_basis = []
    for i in range(2):
        load = pltpu.make_async_copy(
            basis_ref.at[pl.ds(i * half, half)],
            padded.at[pl.ds(BAND + i * half, half)],
            load_sem.at[5 * i + (ny if i else 0)],
        )
        load.start()
        load_basis.append(load)
    load_mass = pltpu.make_async_copy(mass_hbm, mass_ref, load_sem.at[3 + ny])
    load_mass.start()
    load_nb = pltpu.make_async_copy(nb_hbm, nb_ref, load_sem.at[4 + ny])
    load_nb.start()

    peers = [y_right, y_left, partner, *x_near, *z_near]
    barrier = pltpu.get_barrier_semaphore()
    for peer in peers:
        pl.semaphore_signal(barrier, inc=1, device_id=peer, device_id_type=MESH)
    load_blocks = pltpu.make_async_copy(blocks_ref, blocks, load_sem.at[1])
    load_blocks.start()
    load_turn = []
    for i in range(ny + 1):
        load = pltpu.make_async_copy(
            rot_ref.at[
                pl.ds(pl.multiple_of(col_of[i % ny] * width, width), width),
                pl.ds(pl.multiple_of(y * width, width), width),
            ],
            turn.at[pl.ds(i * width, width)],
            load_sem.at[2 + i],
        )
        load.start()
        load_turn.append(load)
    pl.semaphore_wait(barrier, len(peers))

    started = []

    def send(source, target, send_sem, recv_sem, device):
        copy = pltpu.make_async_remote_copy(
            src_ref=source,
            dst_ref=target,
            send_sem=send_sem,
            recv_sem=recv_sem,
            device_id=device,
            device_id_type=MESH,
        )
        copy.start()
        started.append(copy)
        return copy

    low, high = pl.ds(0, half), pl.ds(half, half)
    mine_low, mine_high = pl.ds(BAND, half), pl.ds(BAND + half, half)
    load_basis[0].wait()
    left_first = send(
        padded.at[mine_low], others.at[0, low], y_send.at[0], y_recv.at[0], y_right
    )
    load_basis[1].wait()
    right_first = send(
        padded.at[mine_high], others.at[1, high], y_send.at[1], y_recv.at[1], y_left
    )
    left_second = send(
        padded.at[mine_high], others.at[0, high], y_send.at[2], y_recv.at[2], y_right
    )
    right_second = send(
        padded.at[mine_low], others.at[1, low], y_send.at[3], y_recv.at[3], y_left
    )

    relays = [
        [*z_near, *x_near, partner],
        [z_peers[1], z_peers[nz - 3], *x_near, partner],
        [z_peers[3], z_peers[nz - 5]],
    ]

    def tell(i):
        for peer in relays[i]:
            pl.semaphore_signal(relay.at[i], inc=1, device_id=peer, device_id_type=MESH)

    def hear(i):
        pl.semaphore_wait(relay.at[i], len(relays[i]))

    def weigh(b):
        at = pl.ds(b * size, size)
        column = jnp.broadcast_to(mass_ref[b : b + 1, :], (size, size)).T
        mass_col[at, :] = column
        weights[at, width:] = (column * padded[BAND + b].astype(F32)).astype(BF16)

    tell(0)
    load_mass.wait()
    for b in range(half):
        weigh(b)
    hear(0)
    tell(1)
    for b in range(half, count):
        weigh(b)
    hear(1)
    first_rows, last_rows = pl.ds(BAND, BAND), pl.ds(count, BAND)
    before, after = pl.ds(0, BAND), pl.ds(BAND + count, BAND)
    halo_low = send(
        padded.at[last_rows], padded.at[before], halo_send.at[0], halo_recv.at[0], up
    )
    halo_high = send(
        padded.at[first_rows], padded.at[after], halo_send.at[1], halo_recv.at[1], down
    )
    tell(2)

    def apply(source, store):
        for b in range(count):
            matrix = jnp.concatenate([blocks[b, n] for n in range(3)], axis=1)
            tiles = []
            for n in range(3):
                local = nb_ref[n, b] - place * count + BAND
                local = jnp.minimum(jnp.maximum(local, 0), count + 2 * BAND - 1)
                tiles.append(source[local])
            value = jnp.dot(
                matrix, jnp.concatenate(tiles, axis=0), preferred_element_type=F32
            )
            store(b, value)

    def store_image(b, value):
        weights[pl.ds(b * size, size), :width] = value.astype(BF16)

    load_blocks.wait()
    load_nb.wait()
    halo_low.wait_recv()
    halo_high.wait_recv()
    apply(padded, store_image)
    hear(2)

    def add_gram(which, source, start, length, fresh):
        part = transposed_dot(source, weights[pl.ds(start * size, length * size), :])
        for j in range(2):
            value = part[:, j * width : (j + 1) * width]
            gram[which, j] = value if fresh else gram[which, j] + value

    def some(ref, start, length):
        return ref[pl.ds(start, length)].reshape(length * size, width)

    def pack(which):
        for t in range(width // 8):
            stiff, mass = (gram[which, j, pl.ds(8 * t, 8), :] for j in range(2))
            at = slots * which + t // nx
            for c in range(2):
                rows = slice(4 * c, 4 * c + 4)
                both = jnp.concatenate([stiff[rows], mass[rows]], axis=0)
                plane[2 * (t % nx) + c, at] = both.astype(BF16)

    def plane_sends(at, offset):
        return [
            send(
                plane.at[places[d], at],
                plane_in.at[d, at],
                p_send.at[offset + d],
                p_recv.at[offset + d],
                peer,
            )
            for d, peer in enumerate(q_peers)
        ]

    def plane_sum(at):
        value = plane[q, at].astype(F32)
        for d in range(nq - 1):
            value = value + plane_in[d, at].astype(F32)
        line[at] = value

    at_piece = [pl.ds(slots * i, slots) for i in range(ny)]
    left_first.wait_recv()
    right_first.wait_recv()
    chunks = []
    far_low, far_high = [], []
    for i in range(parts):
        starts = (begins[i], count - begins[i] - pieces[i])
        chunks.append(starts)
        at = pl.ds(starts[0], pieces[i])
        j = 4 + i
        far_low.append(
            send(others.at[0, at], others.at[2, at], y_send.at[j], y_recv.at[j], y_right)
        )
        at = pl.ds(starts[1], pieces[i])
        j = 4 + parts + i
        far_high.append(
            send(others.at[1, at], others.at[2, at], y_send.at[j], y_recv.at[j], y_left)
        )
    left, right, far = (others.at[i] for i in range(3))
    step = count // 4
    for i in range(4):
        add_gram(OWN, some(padded, BAND + i * step, step), i * step, step, i == 0)

    pack(OWN)
    early_hops = plane_sends(at_piece[OWN], 0)
    for i in range(2):
        add_gram(LEFT, some(left, i * step, step), i * step, step, i == 0)
    for i in range(2, 4):
        add_gram(RIGHT, some(right, i * step, step), i * step, step, i == 2)
    for load in load_turn:
        load.wait()
    for i in range(count // 2):
        own = some(padded, BAND + 2 * i, 2)
        if 2 * i < half:
            pair, at = [some(left, 2 * i, 2), own], pl.ds(0, 2 * width)
        else:
            pair, at = [own, some(right, 2 * i, 2)], pl.ds(width, 2 * width)
        turned[pl.ds(2 * i * size, 2 * size), :] = jnp.dot(
            jnp.concatenate(pair, axis=1), turn[at, :], preferred_element_type=F32
        )
    left_second.wait_recv()
    right_second.wait_recv()
    for i in range(2, 4):
        add_gram(LEFT, some(left, i * step, step), i * step, step, False)
    for i in range(2):
        add_gram(RIGHT, some(right, i * step, step), i * step, step, False)

    pack(LEFT)
    early_hops += plane_sends(at_piece[LEFT], nq - 1)
    pack(RIGHT)
    early_hops += plane_sends(at_piece[RIGHT], 2 * (nq - 1))

    sums = jnp.zeros((8, width), F32)

    def far_turn(start, piece, sums):
        at = pl.ds(start * size, piece * size)
        if start < half:
            pair, place_of = [some(right, start, piece), some(far, start, piece)], 2
        else:
            pair, place_of = [some(far, start, piece), some(left, start, piece)], 3
        value = turned[at, :] + jnp.dot(
            jnp.concatenate(pair, axis=1),
            turn[pl.ds(place_of * width, 2 * width), :],
            preferred_element_type=F32,
        )
        turned[at, :] = value
        rimmed[pl.ds(BAND + start, piece)] = value.astype(BF16).reshape(piece, size, width)
        squares = mass_col[at, :] * value * value
        return sums + jnp.sum(squares.reshape(piece * size // 8, 8, width), axis=0)

    rims = []
    quarter = BAND // 2
    def send_rims(done):
        j = 2 + 2 * (done // quarter - 1)
        rims.append(
            send(
                rimmed.at[pl.ds(BAND + done - quarter, quarter)],
                rimmed.at[pl.ds(BAND + count + done - quarter, quarter)],
                halo_send.at[j],
                halo_recv.at[j],
                down,
            )
        )
        rims.append(
            send(
                rimmed.at[pl.ds(BAND + count - done, quarter)],
                rimmed.at[pl.ds(BAND - done, quarter)],
                halo_send.at[j + 1],
                halo_recv.at[j + 1],
                up,
            )
        )

    def far_gram(i):
        for j, start in enumerate(chunks[i]):
            source = some(far, start, pieces[i])
            add_gram(FAR, source, start, pieces[i], i == 0 and j == 0)

    slot_of = [lax.rem(z + d + slots + nz - slots * y, nz) for d in range(nz)]
    line_copies = [
        pltpu.make_async_remote_copy(
            src_ref=line.at[slot_of[d + 1]],
            dst_ref=line_in.at[d],
            send_sem=z_send.at[d],
            recv_sem=z_recv.at[d],
            device_id=peer,
            device_id_type=MESH,
        )
        for d, peer in enumerate(z_peers)
    ]
    far_first = sorted(range(nz - 1), key=lambda d: abs(d + 1 - nz // 2))

    for i in range(parts - 1):
        far_low[i].wait_recv()
        far_high[i].wait_recv()
        for start in chunks[i]:
            sums = far_turn(start, pieces[i], sums)
        done = begins[i] + pieces[i]
        if done in (quarter, BAND):
            send_rims(done)
        far_gram(i)
    early_at, late_at = pl.ds(0, early), pl.ds(early, slots)
    last = parts - 1
    far_low[last].wait_recv()
    far_high[last].wait_recv()
    far_gram(last)
    pack(FAR)
    late_hops = plane_sends(late_at, 3 * (nq - 1))
    for start in chunks[last]:
        sums = far_turn(start, pieces[last], sums)
    sq_own[...] = jnp.sum(sums, axis=0, keepdims=True)
    sq_hops = [
        send(
            sq_own,
            sq_plane_in.at[d],
            p_send.at[4 * (nq - 1) + d],
            p_recv.at[4 * (nq - 1) + d],
            peer,
        )
        for d, peer in enumerate(q_peers)
    ]
    for hop in early_hops:
        hop.wait_recv()
    plane_sum(early_at)
    for d in far_first:
        pl.when(slot_of[d + 1] < early)(line_copies[d].start)
    for hop in sq_hops:
        hop.wait_recv()
    value = sq_own[...]
    for d in range(nq - 1):
        value = value + sq_plane_in[d]
    sq_line[...] = value
    sq_line_hops = [
        send(sq_line, sq_line_in.at[d], z_send.at[nz - 1 + d], z_recv.at[nz - 1 + d], peer)
        for d, peer in enumerate(z_peers)
    ]
    for hop in late_hops:
        hop.wait_recv()
    plane_sum(late_at)
    for d in far_first:
        pl.when(slot_of[d + 1] >= early)(line_copies[d].start)

    def store_product(b, value):
        product[pl.ds(b * size, size), :] = value

    for hop in rims:
        hop.wait_recv()
    apply(rimmed, store_product)

    for hop in sq_line_hops:
        hop.wait_recv()
    norm = sq_line[...]
    for d in range(nz - 1):
        norm = norm + sq_line_in[d]
    scale_out[...] = lax.rsqrt(norm / vertices)
    for copy in line_copies:
        copy.wait_recv()
    value = line[slot_of[0]]
    for d in range(nz - 1):
        value = value + line_in[d]
    gram_out[...] = value / vertices
    for copy in started + line_copies:
        copy.wait_send()


def finish(
    turned, product, scale, gram, basis_out, image_out, stiff_out, mass_out, basis, image, sem
):
    rows = turned.shape[0]
    pieces = 4
    step = rows // pieces
    copies = []
    stiff_out[...] = gram[:4, :]
    mass_out[...] = gram[4:, :]
    for i in range(pieces):
        at = pl.ds(i * step, step)
        for j, (source, held, target) in enumerate(
            ((turned, basis, basis_out), (product, image, image_out))
        ):
            held[at, :] = (source[at, :] * scale[...]).astype(BF16)
            copy = pltpu.make_async_copy(held.at[at], target.at[at], sem.at[2 * i + j])
            copy.start()
            copies.append(copy)
    for copy in copies:
        copy.wait()


def in_hbm(value):
    return pltpu.with_memory_space_constraint(value, pltpu.HBM)


def body(basis_rows, stiff_blocks, block_neighbors, vertex_mass, rotation):
    nz, nx, _ = (lax.axis_size(a) for a in ROWS)
    ny = lax.axis_size("cols")
    rows, width = basis_rows.shape
    count, _, size, _ = stiff_blocks.shape
    pieces = (4, 4, 1, 1)
    parts = len(pieces)
    nq = 2 * nx
    sizes = (nz, nx, ny, count, size, width, pieces)
    reach = (count + 2 * BAND, size, width)
    vmem = pl.BlockSpec(memory_space=pltpu.VMEM)
    hbm = pl.BlockSpec(memory_space=pltpu.HBM)
    dma = pltpu.SemaphoreType.DMA
    turned, product, scale, gram = pl.pallas_call(
        functools.partial(kernel, sizes),
        out_shape=(
            jax.ShapeDtypeStruct((rows, width), F32),
            jax.ShapeDtypeStruct((rows, width), F32),
            jax.ShapeDtypeStruct((1, width), F32),
            jax.ShapeDtypeStruct((8, width), F32),
        ),
        in_specs=[hbm] * 5,
        out_specs=(vmem, vmem, vmem, vmem),
        scratch_shapes=[
            pltpu.VMEM(reach, BF16),
            pltpu.VMEM((3, count, size, width), BF16),
            pltpu.VMEM(reach, BF16),
            pltpu.SMEM((3, count), jnp.int32),
            pltpu.VMEM((count, size), F32),
            pltpu.VMEM((rows, width), F32),
            pltpu.VMEM((rows, 2 * width), BF16),
            pltpu.VMEM(stiff_blocks.shape, BF16),
            pltpu.VMEM(((ny + 1) * width, width), BF16),
            pltpu.VMEM((ny, 2, width, width), F32),
            pltpu.VMEM((nq, nz, 8, width), BF16),
            pltpu.VMEM((nq - 1, nz, 8, width), BF16),
            pltpu.VMEM((nz, 8, width), F32),
            pltpu.VMEM((nz - 1, 8, width), F32),
            pltpu.VMEM((1, width), F32),
            pltpu.VMEM((nq - 1, 1, width), F32),
            pltpu.VMEM((1, width), F32),
            pltpu.VMEM((nz - 1, 1, width), F32),
            pltpu.SemaphoreType.REGULAR((3,)),
            dma((6 + ny,)),
            dma((4 + 2 * parts,)),
            dma((4 + 2 * parts,)),
            dma((6,)),
            dma((6,)),
            dma((5 * (nq - 1),)),
            dma((5 * (nq - 1),)),
            dma((2 * (nz - 1),)),
            dma((2 * (nz - 1),)),
        ],
        compiler_params=pltpu.CompilerParams(
            collective_id=0, has_side_effects=True, vmem_limit_bytes=VMEM_LIMIT
        ),
    )(
        in_hbm(block_neighbors.T),
        in_hbm(basis_rows.reshape(count, size, width)),
        in_hbm(stiff_blocks),
        in_hbm(vertex_mass.reshape(count, size)),
        in_hbm(rotation),
    )
    return pl.pallas_call(
        finish,
        out_shape=(
            jax.ShapeDtypeStruct((rows, width), BF16),
            jax.ShapeDtypeStruct((rows, width), BF16),
            jax.ShapeDtypeStruct((4, width), F32),
            jax.ShapeDtypeStruct((4, width), F32),
        ),
        in_specs=[vmem] * 4,
        out_specs=(hbm, hbm, vmem, vmem),
        scratch_shapes=[
            pltpu.VMEM((rows, width), BF16),
            pltpu.VMEM((rows, width), BF16),
            dma((8,)),
        ],
        compiler_params=pltpu.CompilerParams(vmem_limit_bytes=FINISH_LIMIT),
    )(turned, product, scale, gram)


def solution(mesh):
    split = Mesh(
        mesh.devices.reshape(16, 4, 2, mesh.shape["cols"]), ("rows_0", "rows_1", "rows_2", "cols")
    )
    in_specs = (P(ROWS, "cols"), P(ROWS, None, None, None), P(ROWS, None), P(ROWS), P())
    out_specs = (P(ROWS, "cols"), P(ROWS, "cols"), P(ROWS, "cols"), P(ROWS, "cols"))
    return jax.shard_map(body, mesh=split, in_specs=in_specs, out_specs=out_specs, check_vma=False)
```

```python
import functools

import jax
import jax.numpy as jnp
from jax import lax
from jax.experimental import pallas as pl
from jax.experimental.pallas import tpu as pltpu
from jax.sharding import Mesh
from jax.sharding import PartitionSpec as P

BAND = 8
ROWS = ("rows_0", "rows_1", "rows_2")
MESH = pl.DeviceIdType.MESH
F32 = jnp.float32
BF16 = jnp.bfloat16
LEFT, OWN, RIGHT, FAR = 0, 1, 2, 3
VMEM_LIMIT = 24 * 1024 * 1024
FINISH_LIMIT = 16 * 1024 * 1024


def transposed_dot(left, right):
    return lax.dot_general(left, right, (((0,), (0,)), ((), ())), preferred_element_type=F32)


def kernel(
    sizes,
    nb_hbm,
    basis_ref,
    blocks_ref,
    mass_hbm,
    rot_ref,
    turned,
    product,
    scale_out,
    gram_out,
    padded,
    others,
    rimmed,
    nb_ref,
    mass_ref,
    mass_col,
    weights,
    blocks,
    turn,
    gram,
    plane,
    plane_in,
    line,
    line_in,
    sq_own,
    sq_plane_in,
    sq_line,
    sq_line_in,
    relay,
    load_sem,
    y_send,
    y_recv,
    halo_send,
    halo_recv,
    p_send,
    p_recv,
    z_send,
    z_recv,
):
    nz, nx, ny, count, size, width, pieces = sizes
    z, x, k = (lax.axis_index(a) for a in ROWS)
    y = lax.axis_index("cols")
    half = count // 2
    parts = len(pieces)
    begins = [sum(pieces[:i]) for i in range(parts)]
    total = nz * nx * 2
    nq = 2 * nx
    q = 2 * x + k
    place = z * nq + q
    vertices = total * count * size
    slots = nz // ny
    early = nz - slots

    def row_device(index):
        index = lax.rem(index + total, total)
        return {
            "rows_0": lax.div(index, nq),
            "rows_1": lax.rem(lax.div(index, 2), nx),
            "rows_2": lax.rem(index, 2),
        }

    def along(axis, mine, length, step):
        return {axis: lax.rem(mine + length + step, length)}

    up, down = row_device(place + 1), row_device(place - 1)
    y_right, y_left = along("cols", y, ny, 1), along("cols", y, ny, -1)
    partner = {"rows_2": 1 - k}
    x_near = [along("rows_1", x, nx, d) for d in (1, -1)]
    z_near = [along("rows_0", z, nz, d) for d in (1, -1)]
    places = [lax.rem(q + d, nq) for d in range(1, nq)]
    q_peers = [{"rows_1": lax.div(p, 2), "rows_2": lax.rem(p, 2)} for p in places]
    z_peers = [along("rows_0", z, nz, d) for d in range(1, nz)]
    col_of = [lax.rem(y + ny - 1 + i, ny) for i in range(ny)]

    load_basis = []
    for i in range(2):
        load = pltpu.make_async_copy(
            basis_ref.at[pl.ds(i * half, half)],
            padded.at[pl.ds(BAND + i * half, half)],
            load_sem.at[5 * i + (ny if i else 0)],
        )
        load.start()
        load_basis.append(load)
    load_mass = pltpu.make_async_copy(mass_hbm, mass_ref, load_sem.at[3 + ny])
    load_mass.start()
    load_nb = pltpu.make_async_copy(nb_hbm, nb_ref, load_sem.at[4 + ny])
    load_nb.start()

    peers = [y_right, y_left, partner, *x_near, *z_near]
    barrier = pltpu.get_barrier_semaphore()
    for peer in peers:
        pl.semaphore_signal(barrier, inc=1, device_id=peer, device_id_type=MESH)
    load_blocks = pltpu.make_async_copy(blocks_ref, blocks, load_sem.at[1])
    load_blocks.start()
    load_turn = []
    for i in range(ny + 1):
        load = pltpu.make_async_copy(
            rot_ref.at[
                pl.ds(pl.multiple_of(col_of[i % ny] * width, width), width),
                pl.ds(pl.multiple_of(y * width, width), width),
            ],
            turn.at[pl.ds(i * width, width)],
            load_sem.at[2 + i],
        )
        load.start()
        load_turn.append(load)
    pl.semaphore_wait(barrier, len(peers))

    started = []

    def send(source, target, send_sem, recv_sem, device):
        copy = pltpu.make_async_remote_copy(
            src_ref=source,
            dst_ref=target,
            send_sem=send_sem,
            recv_sem=recv_sem,
            device_id=device,
            device_id_type=MESH,
        )
        copy.start()
        started.append(copy)
        return copy

    low, high = pl.ds(0, half), pl.ds(half, half)
    mine_low, mine_high = pl.ds(BAND, half), pl.ds(BAND + half, half)
    load_basis[0].wait()
    left_first = send(
        padded.at[mine_low], others.at[0, low], y_send.at[0], y_recv.at[0], y_right
    )
    load_basis[1].wait()
    right_first = send(
        padded.at[mine_high], others.at[1, high], y_send.at[1], y_recv.at[1], y_left
    )
    left_second = send(
        padded.at[mine_high], others.at[0, high], y_send.at[2], y_recv.at[2], y_right
    )
    right_second = send(
        padded.at[mine_low], others.at[1, low], y_send.at[3], y_recv.at[3], y_left
    )

    relays = [
        [*z_near, *x_near, partner],
        [z_peers[1], z_peers[nz - 3], *x_near, partner],
        [z_peers[3], z_peers[nz - 5]],
    ]

    def tell(i):
        for peer in relays[i]:
            pl.semaphore_signal(relay.at[i], inc=1, device_id=peer, device_id_type=MESH)

    def hear(i):
        pl.semaphore_wait(relay.at[i], len(relays[i]))

    def weigh(b):
        at = pl.ds(b * size, size)
        column = jnp.broadcast_to(mass_ref[b : b + 1, :], (size, size)).T
        mass_col[at, :] = column
        weights[at, width:] = (column * padded[BAND + b].astype(F32)).astype(BF16)

    tell(0)
    load_mass.wait()
    for b in range(half):
        weigh(b)
    hear(0)
    tell(1)
    for b in range(half, count):
        weigh(b)
    hear(1)
    first_rows, last_rows = pl.ds(BAND, BAND), pl.ds(count, BAND)
    before, after = pl.ds(0, BAND), pl.ds(BAND + count, BAND)
    halo_low = send(
        padded.at[last_rows], padded.at[before], halo_send.at[0], halo_recv.at[0], up
    )
    halo_high = send(
        padded.at[first_rows], padded.at[after], halo_send.at[1], halo_recv.at[1], down
    )
    tell(2)

    def apply(source, store):
        for b in range(count):
            matrix = jnp.concatenate([blocks[b, n] for n in range(3)], axis=1)
            tiles = []
            for n in range(3):
                local = nb_ref[n, b] - place * count + BAND
                local = jnp.minimum(jnp.maximum(local, 0), count + 2 * BAND - 1)
                tiles.append(source[local])
            value = jnp.dot(
                matrix, jnp.concatenate(tiles, axis=0), preferred_element_type=F32
            )
            store(b, value)

    def store_image(b, value):
        weights[pl.ds(b * size, size), :width] = value.astype(BF16)

    load_blocks.wait()
    load_nb.wait()
    halo_low.wait_recv()
    halo_high.wait_recv()
    apply(padded, store_image)
    hear(2)

    def add_gram(which, source, start, length, fresh):
        part = transposed_dot(source, weights[pl.ds(start * size, length * size), :])
        for j in range(2):
            value = part[:, j * width : (j + 1) * width]
            gram[which, j] = value if fresh else gram[which, j] + value

    def some(ref, start, length):
        return ref[pl.ds(start, length)].reshape(length * size, width)

    def pack(which):
        for t in range(width // 8):
            stiff, mass = (gram[which, j, pl.ds(8 * t, 8), :] for j in range(2))
            at = slots * which + t // nx
            for c in range(2):
                rows = slice(4 * c, 4 * c + 4)
                both = jnp.concatenate([stiff[rows], mass[rows]], axis=0)
                plane[2 * (t % nx) + c, at] = both.astype(BF16)

    def plane_sends(at, offset):
        return [
            send(
                plane.at[places[d], at],
                plane_in.at[d, at],
                p_send.at[offset + d],
                p_recv.at[offset + d],
                peer,
            )
            for d, peer in enumerate(q_peers)
        ]

    def plane_sum(at):
        value = plane[q, at].astype(F32)
        for d in range(nq - 1):
            value = value + plane_in[d, at].astype(F32)
        line[at] = value

    at_piece = [pl.ds(slots * i, slots) for i in range(ny)]
    left_first.wait_recv()
    right_first.wait_recv()
    chunks = []
    far_low, far_high = [], []
    for i in range(parts):
        starts = (begins[i], count - begins[i] - pieces[i])
        chunks.append(starts)
        at = pl.ds(starts[0], pieces[i])
        j = 4 + i
        far_low.append(
            send(others.at[0, at], others.at[2, at], y_send.at[j], y_recv.at[j], y_right)
        )
        at = pl.ds(starts[1], pieces[i])
        j = 4 + parts + i
        far_high.append(
            send(others.at[1, at], others.at[2, at], y_send.at[j], y_recv.at[j], y_left)
        )
    left, right, far = (others.at[i] for i in range(3))
    step = count // 4
    for i in range(4):
        add_gram(OWN, some(padded, BAND + i * step, step), i * step, step, i == 0)

    pack(OWN)
    early_hops = plane_sends(at_piece[OWN], 0)
    for i in range(2):
        add_gram(LEFT, some(left, i * step, step), i * step, step, i == 0)
    for i in range(2, 4):
        add_gram(RIGHT, some(right, i * step, step), i * step, step, i == 2)
    for load in load_turn:
        load.wait()
    for i in range(count // 2):
        own = some(padded, BAND + 2 * i, 2)
        if 2 * i < half:
            pair, at = [some(left, 2 * i, 2), own], pl.ds(0, 2 * width)
        else:
            pair, at = [own, some(right, 2 * i, 2)], pl.ds(width, 2 * width)
        turned[pl.ds(2 * i * size, 2 * size), :] = jnp.dot(
            jnp.concatenate(pair, axis=1), turn[at, :], preferred_element_type=F32
        )
    left_second.wait_recv()
    right_second.wait_recv()
    for i in range(2, 4):
        add_gram(LEFT, some(left, i * step, step), i * step, step, False)
    for i in range(2):
        add_gram(RIGHT, some(right, i * step, step), i * step, step, False)

    pack(LEFT)
    early_hops += plane_sends(at_piece[LEFT], nq - 1)
    pack(RIGHT)
    early_hops += plane_sends(at_piece[RIGHT], 2 * (nq - 1))

    sums = jnp.zeros((8, width), F32)

    def far_turn(start, piece, sums):
        at = pl.ds(start * size, piece * size)
        if start < half:
            pair, place_of = [some(right, start, piece), some(far, start, piece)], 2
        else:
            pair, place_of = [some(far, start, piece), some(left, start, piece)], 3
        value = turned[at, :] + jnp.dot(
            jnp.concatenate(pair, axis=1),
            turn[pl.ds(place_of * width, 2 * width), :],
            preferred_element_type=F32,
        )
        turned[at, :] = value
        rimmed[pl.ds(BAND + start, piece)] = value.astype(BF16).reshape(piece, size, width)
        squares = mass_col[at, :] * value * value
        return sums + jnp.sum(squares.reshape(piece * size // 8, 8, width), axis=0)

    rims = []
    quarter = BAND // 2
    def send_rims(done):
        j = 2 + 2 * (done // quarter - 1)
        rims.append(
            send(
                rimmed.at[pl.ds(BAND + done - quarter, quarter)],
                rimmed.at[pl.ds(BAND + count + done - quarter, quarter)],
                halo_send.at[j],
                halo_recv.at[j],
                down,
            )
        )
        rims.append(
            send(
                rimmed.at[pl.ds(BAND + count - done, quarter)],
                rimmed.at[pl.ds(BAND - done, quarter)],
                halo_send.at[j + 1],
                halo_recv.at[j + 1],
                up,
            )
        )

    def far_gram(i):
        length = pieces[i]
        source = jnp.concatenate([some(far, start, length) for start in chunks[i]], axis=0)
        right_side = jnp.concatenate(
            [weights[pl.ds(start * size, length * size), :] for start in chunks[i]], axis=0
        )
        part = transposed_dot(source, right_side)
        for j in range(2):
            value = part[:, j * width : (j + 1) * width]
            gram[FAR, j] = value if i == 0 else gram[FAR, j] + value

    slot_of = [lax.rem(z + d + slots + nz - slots * y, nz) for d in range(nz)]
    line_copies = [
        pltpu.make_async_remote_copy(
            src_ref=line.at[slot_of[d + 1]],
            dst_ref=line_in.at[d],
            send_sem=z_send.at[d],
            recv_sem=z_recv.at[d],
            device_id=peer,
            device_id_type=MESH,
        )
        for d, peer in enumerate(z_peers)
    ]
    far_first = sorted(range(nz - 1), key=lambda d: abs(d + 1 - nz // 2))

    for i in range(parts - 1):
        far_low[i].wait_recv()
        far_high[i].wait_recv()
        for start in chunks[i]:
            sums = far_turn(start, pieces[i], sums)
        done = begins[i] + pieces[i]
        if done in (quarter, BAND):
            send_rims(done)
        far_gram(i)
    early_at, late_at = pl.ds(0, early), pl.ds(early, slots)
    last = parts - 1
    far_low[last].wait_recv()
    far_high[last].wait_recv()
    far_gram(last)
    pack(FAR)
    late_hops = plane_sends(late_at, 3 * (nq - 1))
    for start in chunks[last]:
        sums = far_turn(start, pieces[last], sums)
    sq_own[...] = jnp.sum(sums, axis=0, keepdims=True)
    sq_hops = [
        send(
            sq_own,
            sq_plane_in.at[d],
            p_send.at[4 * (nq - 1) + d],
            p_recv.at[4 * (nq - 1) + d],
            peer,
        )
        for d, peer in enumerate(q_peers)
    ]
    for hop in early_hops:
        hop.wait_recv()
    plane_sum(early_at)
    for d in far_first:
        pl.when(slot_of[d + 1] < early)(line_copies[d].start)
    for hop in sq_hops:
        hop.wait_recv()
    value = sq_own[...]
    for d in range(nq - 1):
        value = value + sq_plane_in[d]
    sq_line[...] = value
    sq_line_hops = [
        send(sq_line, sq_line_in.at[d], z_send.at[nz - 1 + d], z_recv.at[nz - 1 + d], peer)
        for d, peer in enumerate(z_peers)
    ]
    for hop in late_hops:
        hop.wait_recv()
    plane_sum(late_at)
    for d in far_first:
        pl.when(slot_of[d + 1] >= early)(line_copies[d].start)

    def store_product(b, value):
        product[pl.ds(b * size, size), :] = value

    for hop in rims:
        hop.wait_recv()
    apply(rimmed, store_product)

    for hop in sq_line_hops:
        hop.wait_recv()
    norm = sq_line[...]
    for d in range(nz - 1):
        norm = norm + sq_line_in[d]
    scale_out[...] = lax.rsqrt(norm / vertices)
    for copy in line_copies:
        copy.wait_recv()
    value = line[slot_of[0]]
    for d in range(nz - 1):
        value = value + line_in[d]
    gram_out[...] = value / vertices
    for copy in started + line_copies:
        copy.wait_send()


def finish(
    turned, product, scale, gram, basis_out, image_out, stiff_out, mass_out, basis, image, sem
):
    rows = turned.shape[0]
    pieces = 4
    step = rows // pieces
    copies = []
    stiff_out[...] = gram[:4, :]
    mass_out[...] = gram[4:, :]
    for i in range(pieces):
        at = pl.ds(i * step, step)
        for j, (source, held, target) in enumerate(
            ((turned, basis, basis_out), (product, image, image_out))
        ):
            held[at, :] = (source[at, :] * scale[...]).astype(BF16)
            copy = pltpu.make_async_copy(held.at[at], target.at[at], sem.at[2 * i + j])
            copy.start()
            copies.append(copy)
    for copy in copies:
        copy.wait()


def in_hbm(value):
    return pltpu.with_memory_space_constraint(value, pltpu.HBM)


def body(basis_rows, stiff_blocks, block_neighbors, vertex_mass, rotation):
    nz, nx, _ = (lax.axis_size(a) for a in ROWS)
    ny = lax.axis_size("cols")
    rows, width = basis_rows.shape
    count, _, size, _ = stiff_blocks.shape
    pieces = (4, 4, 1, 1)
    parts = len(pieces)
    nq = 2 * nx
    sizes = (nz, nx, ny, count, size, width, pieces)
    reach = (count + 2 * BAND, size, width)
    vmem = pl.BlockSpec(memory_space=pltpu.VMEM)
    hbm = pl.BlockSpec(memory_space=pltpu.HBM)
    dma = pltpu.SemaphoreType.DMA
    turned, product, scale, gram = pl.pallas_call(
        functools.partial(kernel, sizes),
        out_shape=(
            jax.ShapeDtypeStruct((rows, width), F32),
            jax.ShapeDtypeStruct((rows, width), F32),
            jax.ShapeDtypeStruct((1, width), F32),
            jax.ShapeDtypeStruct((8, width), F32),
        ),
        in_specs=[hbm] * 5,
        out_specs=(vmem, vmem, vmem, vmem),
        scratch_shapes=[
            pltpu.VMEM(reach, BF16),
            pltpu.VMEM((3, count, size, width), BF16),
            pltpu.VMEM(reach, BF16),
            pltpu.SMEM((3, count), jnp.int32),
            pltpu.VMEM((count, size), F32),
            pltpu.VMEM((rows, width), F32),
            pltpu.VMEM((rows, 2 * width), BF16),
            pltpu.VMEM(stiff_blocks.shape, BF16),
            pltpu.VMEM(((ny + 1) * width, width), BF16),
            pltpu.VMEM((ny, 2, width, width), F32),
            pltpu.VMEM((nq, nz, 8, width), BF16),
            pltpu.VMEM((nq - 1, nz, 8, width), BF16),
            pltpu.VMEM((nz, 8, width), F32),
            pltpu.VMEM((nz - 1, 8, width), F32),
            pltpu.VMEM((1, width), F32),
            pltpu.VMEM((nq - 1, 1, width), F32),
            pltpu.VMEM((1, width), F32),
            pltpu.VMEM((nz - 1, 1, width), F32),
            pltpu.SemaphoreType.REGULAR((3,)),
            dma((6 + ny,)),
            dma((4 + 2 * parts,)),
            dma((4 + 2 * parts,)),
            dma((6,)),
            dma((6,)),
            dma((5 * (nq - 1),)),
            dma((5 * (nq - 1),)),
            dma((2 * (nz - 1),)),
            dma((2 * (nz - 1),)),
        ],
        compiler_params=pltpu.CompilerParams(
            collective_id=0, has_side_effects=True, vmem_limit_bytes=VMEM_LIMIT
        ),
    )(
        in_hbm(block_neighbors.T),
        in_hbm(basis_rows.reshape(count, size, width)),
        in_hbm(stiff_blocks),
        in_hbm(vertex_mass.reshape(count, size)),
        in_hbm(rotation),
    )
    return pl.pallas_call(
        finish,
        out_shape=(
            jax.ShapeDtypeStruct((rows, width), BF16),
            jax.ShapeDtypeStruct((rows, width), BF16),
            jax.ShapeDtypeStruct((4, width), F32),
            jax.ShapeDtypeStruct((4, width), F32),
        ),
        in_specs=[vmem] * 4,
        out_specs=(hbm, hbm, vmem, vmem),
        scratch_shapes=[
            pltpu.VMEM((rows, width), BF16),
            pltpu.VMEM((rows, width), BF16),
            dma((8,)),
        ],
        compiler_params=pltpu.CompilerParams(vmem_limit_bytes=FINISH_LIMIT),
    )(turned, product, scale, gram)


def solution(mesh):
    split = Mesh(
        mesh.devices.reshape(16, 4, 2, mesh.shape["cols"]), ("rows_0", "rows_1", "rows_2", "cols")
    )
    in_specs = (P(ROWS, "cols"), P(ROWS, None, None, None), P(ROWS, None), P(ROWS), P())
    out_specs = (P(ROWS, "cols"), P(ROWS, "cols"), P(ROWS, "cols"), P(ROWS, "cols"))
    return jax.shard_map(body, mesh=split, in_specs=in_specs, out_specs=out_specs, check_vma=False)
```
